256 devices in a mesh: dp: 32 (over y, z), neg: 8 (over x, core).
Axes of the slice: x: 4, y: 4, z: 8, core: 2. Of those that a mesh axis runs over, the one named last changes fastest.
Arguments:
- query_features: bfloat16 [65536, 512], P(('dp', 'neg')), may hold values from -8 to 8
- positive_features: bfloat16 [65536, 512], P(('dp', 'neg')), may hold values from -6 to 6
- negative_features: bfloat16 [16384, 512], P(('neg', 'dp')), may hold values from -6 to 6
- positive_ids: int32 [65536], P('dp'), may hold values from 0 to 8191, as said below
- positive_counts: int32 [65536], P(('dp', 'neg')), may hold values from 1 to 16
- negative_ids: int32 [16384], P('neg'), may hold values from 0 to 4095, as said below
- negative_counts: int32 [16384], P('neg'), may hold values from 64 to 4096
- query_first: bfloat16 [512, 1024], replicated, may hold values from -0.25 to 0.25
- query_second: bfloat16 [1024, 512], replicated, may hold values from -0.1875 to 0.1875
- query_third: bfloat16 [512, 256], replicated, may hold values from -0.25 to 0.25
- item_first: bfloat16 [512, 1024], replicated, may hold values from -0.25 to 0.25
- item_second: bfloat16 [1024, 512], replicated, may hold values from -0.1875 to 0.1875
- item_third: bfloat16 [512, 256], replicated, may hold values from -0.25 to 0.25
Outputs:
- mean_loss: float32 [], replicated
- clipped_query_first: float32 [512, 1024], P('dp')
- clipped_query_second: float32 [1024, 512], P('dp')
- clipped_query_third: float32 [512, 256], P('dp')
- clipped_item_first: float32 [512, 1024], P('dp')
- clipped_item_second: float32 [1024, 512], P('dp')
- clipped_item_third: float32 [512, 256], P('dp')
The draws below stay inside these ranges and needn't reach their ends.
Inputs may be any that keep to these rules, and one draw needn't show every extreme that they name: `negative_ids`: ids of the sampled negatives; one id may stand for several negatives. `positive_ids`: A query's positive id may equal the ids of some negatives; those negatives are left out of that query's denominator.
All inputs are finite; a program needn't handle non-finite values.
Results may differ from the reference program's by a relative error of at most 0.0075.
Values may be sent and summed in bfloat16 or wider, within the bound.
A program may use at most 128 MiB of HBM per device.

```python
import math
import jax
import jax.numpy as jnp
from jax import lax

FIN = 512
H1 = 1024
H2 = 512
E = 256
NEG = 16384
QUERIES = 65536


def draw_query_features(key, part):
    noise_key, mean_key, scale_key = jax.random.split(key, 3)
    values = jax.random.normal(noise_key, (QUERIES, FIN), jnp.float32)
    return jnp.clip(values, -8.0, 8.0).astype(jnp.bfloat16)


def draw_item_ids(key):
    base = jax.random.fold_in(key, 91)
    pool_key, pick_key, fresh_key, hit_key = jax.random.split(base, 4)
    negatives = jax.random.randint(pool_key, (NEG,), 0, NEG // 4, jnp.int32)
    negatives = negatives.at[0].set(NEG // 4 - 1).at[1].set(0)
    picked = jax.random.randint(pick_key, (QUERIES,), 0, NEG, jnp.int32)
    fresh = jax.random.randint(fresh_key, (QUERIES,), NEG // 4, NEG // 2, jnp.int32)
    choose_hit = jax.random.randint(hit_key, (QUERIES,), 0, 2, jnp.int32)
    positives = jnp.where(choose_hit == 0, negatives[picked], fresh)
    positives = positives.at[0].set(NEG // 2 - 1).at[1].set(0)
    return (negatives, positives)


def draw_negative_ids(key, part):
    return draw_item_ids(key)[0]


def draw_positive_ids(key, part):
    return draw_item_ids(key)[1]


def blocked_counts(key, total, block_rows, low_power, high_power):
    level_key, fine_key = jax.random.split(key)
    levels = jax.random.randint(level_key, (total // block_rows + 1,), low_power, high_power + 1, jnp.int32)
    powers = jnp.left_shift(jnp.ones_like(levels), levels)
    which = jnp.arange(total, dtype=jnp.int32) // block_rows
    base = powers[which]
    fine = jax.random.randint(fine_key, (total,), 0, 65536, jnp.int32) % base
    return base + fine


def draw_negative_counts(key, part):
    counts = blocked_counts(jax.random.fold_in(key, 17), NEG, 256, 6, 11)
    return counts.at[0].set(4096).at[1].set(64)


def draw_positive_counts(key, part):
    counts = blocked_counts(jax.random.fold_in(key, 23), QUERIES, 64, 0, 3)
    return counts.at[0].set(16).at[1].set(1)


def block_scale(key, shape, pieces, least, top_value):
    loudness = 1.0
    for dim, parts in pieces:
        heights = jax.random.uniform(jax.random.fold_in(jax.random.fold_in(key, 6), dim), (parts,), jnp.float32, least / len(pieces), top_value / len(pieces))
        loudness = loudness * jnp.repeat(jnp.exp(heights), shape[dim] // parts).reshape((-1,) + (1,) * (len(shape) - 1 - dim))
    return loudness


def bell_draw(key, shape, scale, limit, shards=(), kind=jnp.bfloat16):
    gain = block_scale(key, shape, shards, -0.22, 0.18) if shards else 1.0
    drawn = jax.random.normal(key, shape, jnp.float32) * scale * gain
    return jnp.minimum(jnp.maximum(drawn, -limit), limit).astype(kind)


def setup_inputs(seed: int = 0) -> dict:
    streams_of = jax.random.split(jax.random.key(seed), 14)
    query_features = draw_query_features(jax.random.fold_in(streams_of[13], 71), 0)
    positive_features = bell_draw(streams_of[1], (QUERIES, FIN), 1.0, 6.0, ((0, 256),))
    negative_features = bell_draw(streams_of[2], (NEG, FIN), 1.0, 6.0, ((0, 256),))
    positive_ids = draw_positive_ids(jax.random.fold_in(streams_of[13], 71), 0)
    positive_counts = draw_positive_counts(jax.random.fold_in(streams_of[13], 71), 0)
    negative_ids = draw_negative_ids(jax.random.fold_in(streams_of[13], 71), 0)
    negative_counts = draw_negative_counts(jax.random.fold_in(streams_of[13], 71), 0)
    query_first = bell_draw(streams_of[7], (FIN, H1), FIN ** -0.5, 0.25)
    query_second = bell_draw(streams_of[8], (H1, H2), H1 ** -0.5, 0.1875)
    query_third = bell_draw(streams_of[9], (H2, E), H2 ** -0.5, 0.25)
    item_first = bell_draw(streams_of[10], (FIN, H1), FIN ** -0.5, 0.25)
    item_second = bell_draw(streams_of[11], (H1, H2), H1 ** -0.5, 0.1875)
    item_third = bell_draw(streams_of[12], (H2, E), H2 ** -0.5, 0.25)
    return dict(query_features=query_features, positive_features=positive_features, negative_features=negative_features, positive_ids=positive_ids, positive_counts=positive_counts, negative_ids=negative_ids, negative_counts=negative_counts, query_first=query_first, query_second=query_second, query_third=query_third, item_first=item_first, item_second=item_second, item_third=item_third)


inv_temp = 20.0
clip_norm = 256.0

def silu_slope(pre):
    sigma = jax.nn.sigmoid(pre)
    return sigma * (1.0 + pre * (1.0 - sigma))

def contract_rows(left, right):
    return lax.dot_general(left, right, (((0,), (0,)), ((), ())), preferred_element_type=jnp.float32)

def contract_cols(left, right):
    return lax.dot_general(left, right, (((1,), (1,)), ((), ())), preferred_element_type=jnp.float32)

def tower_forward(features, first, second, third):
    first_pre = jnp.dot(features, first, preferred_element_type=jnp.float32)
    first_act = jax.nn.silu(first_pre).astype(jnp.bfloat16)
    second_pre = jnp.dot(first_act, second, preferred_element_type=jnp.float32)
    second_act = jax.nn.silu(second_pre).astype(jnp.bfloat16)
    embedding = jnp.dot(second_act, third, preferred_element_type=jnp.float32)
    inv_norm = lax.rsqrt(lax.optimization_barrier(jnp.sum(embedding * embedding, axis=1, keepdims=True)) + 1.0)
    unit = (embedding * inv_norm).astype(jnp.bfloat16)
    return ((first_pre, first_act, second_pre, second_act, embedding, inv_norm), unit)

def tower_backward(features, second, third, saved, unit_grad):
    first_pre, first_act, second_pre, second_act, embedding, inv_norm = saved
    along = lax.optimization_barrier(jnp.sum(embedding * unit_grad, axis=1, keepdims=True))
    embed_grad = (inv_norm * unit_grad - inv_norm * inv_norm * inv_norm * embedding * along).astype(jnp.bfloat16)
    third_grad = contract_rows(second_act, embed_grad)
    second_slope = (contract_cols(embed_grad, third) * silu_slope(second_pre)).astype(jnp.bfloat16)
    second_grad = contract_rows(first_act, second_slope)
    first_slope = (contract_cols(second_slope, second) * silu_slope(first_pre)).astype(jnp.bfloat16)
    first_grad = contract_rows(features, first_slope)
    return (first_grad, second_grad, third_grad)

def reference(query_features, positive_features, negative_features, positive_ids, positive_counts, negative_ids, negative_counts, query_first, query_second, query_third, item_first, item_second, item_third):
    query_saved, query_unit = tower_forward(query_features, query_first, query_second, query_third)
    item_features = jnp.concatenate([positive_features, negative_features], axis=0)
    item_saved, item_unit = tower_forward(item_features, item_first, item_second, item_third)
    positive_unit = item_unit[:QUERIES]
    negative_unit = item_unit[QUERIES:]
    negative_log = jnp.log(negative_counts.astype(jnp.float32))
    positive_logit = lax.optimization_barrier(jnp.sum(query_unit.astype(jnp.float32) * positive_unit.astype(jnp.float32), axis=1)) * inv_temp - jnp.log(positive_counts.astype(jnp.float32))
    block_rows = math.gcd(QUERIES, 2048)
    blocks = QUERIES // block_rows

    def block_step(carry, inputs):
        negative_sum, loss_sum = carry
        query_block, positive_block, logit_block, ids_block = inputs
        scores = contract_cols(query_block, negative_unit) * inv_temp - negative_log[None, :]
        weights = jnp.where(ids_block[:, None] != negative_ids[None, :], jnp.exp(scores), 0.0)
        positive_exp = jnp.exp(logit_block)
        denom = positive_exp + lax.optimization_barrier(jnp.sum(weights, axis=1))
        loss_sum = loss_sum + jnp.sum(jnp.log(denom) - logit_block)
        softmax_weights = (weights / denom[:, None]).astype(jnp.bfloat16)
        positive_slope = positive_exp / denom - 1.0
        query_grad = (jnp.dot(softmax_weights, negative_unit, preferred_element_type=jnp.float32) + positive_slope[:, None] * positive_block.astype(jnp.float32)) * inv_temp
        positive_grad = positive_slope[:, None] * query_block.astype(jnp.float32) * inv_temp
        negative_sum = negative_sum + contract_rows(softmax_weights, query_block)
        return ((negative_sum, loss_sum), (query_grad, positive_grad))
    inputs = (query_unit.reshape(blocks, block_rows, E), positive_unit.reshape(blocks, block_rows, E), positive_logit.reshape(blocks, block_rows), positive_ids.reshape(blocks, block_rows))
    initial = (jnp.zeros((NEG, E), jnp.float32), jnp.zeros((), jnp.float32))
    (negative_sum, loss_sum), (query_grad, positive_grad) = lax.scan(block_step, initial, inputs)
    query_grad = query_grad.reshape(QUERIES, E)
    item_grad = jnp.concatenate([positive_grad.reshape(QUERIES, E), negative_sum * inv_temp], axis=0)
    query_grads = tower_backward(query_features, query_second, query_third, query_saved, query_grad)
    item_grads = tower_backward(item_features, item_second, item_third, item_saved, item_grad)
    gradients = query_grads + item_grads
    squares = jnp.zeros((), jnp.float32)
    for gradient in gradients:
        squares = squares + jnp.sum(gradient * gradient)
    grad_norm = jnp.sqrt(squares)
    clip_factor = clip_norm / jnp.maximum(grad_norm, clip_norm)
    mean_loss = loss_sum / QUERIES
    return (mean_loss, gradients[0] * clip_factor, gradients[1] * clip_factor, gradients[2] * clip_factor, gradients[3] * clip_factor, gradients[4] * clip_factor, gradients[5] * clip_factor)
```

```python
import jax
import jax.numpy as jnp
from jax import lax
from jax.experimental import pallas as pl
from jax.experimental.pallas import tpu as pltpu
from jax.sharding import Mesh
from jax.sharding import PartitionSpec as P

NEG = ("neg_0", "neg_1")
DP = ("dp_0", "dp_1")
DP_NEG = ("dp_0", "dp_1", "neg_0", "neg_1")
NEG_DP = ("neg_0", "neg_1", "dp_0", "dp_1")
AX_Y, AX_Z, AX_X, AX_C = "dp_0", "dp_1", "neg_0", "neg_1"
MESH = pl.DeviceIdType.MESH
F32 = jnp.float32
BF16 = jnp.bfloat16

inv_temp = 20.0
clip_norm = 256.0


def laid_out(tiles, dim):
    tiles = jnp.moveaxis(tiles, 0, dim)
    shape = tiles.shape
    return tiles.reshape(*shape[:dim], shape[dim] * shape[dim + 1], *shape[dim + 2 :])


def from_everyone(array, axis):
    copies = jnp.broadcast_to(array, (lax.axis_size(axis), *array.shape))
    return lax.all_to_all(copies, axis, split_axis=0, concat_axis=0, tiled=True)


def collect(array, axis, dim):
    return laid_out(from_everyone(array, axis), dim)


def over_copies(array, axis):
    return from_everyone(array, axis).sum(axis=0)


def cut_along(array, dim, length):
    shape = array.shape
    tiles = array.reshape(*shape[:dim], length, shape[dim] // length, *shape[dim + 1 :])
    return jnp.moveaxis(tiles, dim, 0)


def sent_and_summed(array, axis, dim):
    length = lax.axis_size(axis)
    tiles = lax.all_to_all(cut_along(array, dim, length), axis, 0, 0, tiled=True)
    return jnp.sum(tiles, axis=0)


def own_rows_2(so_far, axes):
    for axis in axes:
        so_far = lax.psum_scatter(so_far, axis, scatter_dimension=0, tiled=True)
    return so_far


def silu_slope(pre):
    sigma = jax.nn.sigmoid(pre)
    return sigma * (1.0 + pre * (1.0 - sigma))


def contract_rows(left, right):
    return lax.dot_general(
        left, right, (((0,), (0,)), ((), ())), preferred_element_type=jnp.float32
    )


def contract_cols(left, right):
    return lax.dot_general(
        left, right, (((1,), (1,)), ((), ())), preferred_element_type=jnp.float32
    )


def tower_forward(features, first, second, third):
    first_pre = jnp.dot(features, first, preferred_element_type=jnp.float32)
    first_act = jax.nn.silu(first_pre).astype(jnp.bfloat16)
    second_pre = jnp.dot(first_act, second, preferred_element_type=jnp.float32)
    second_act = jax.nn.silu(second_pre).astype(jnp.bfloat16)
    embedding = jnp.dot(second_act, third, preferred_element_type=jnp.float32)
    inv_norm = lax.rsqrt(jnp.sum(embedding * embedding, axis=1, keepdims=True) + 1.0)
    unit = (embedding * inv_norm).astype(jnp.bfloat16)
    return ((first_pre, first_act, second_pre, second_act, embedding, inv_norm), unit)


def tower_backward(features, second, third, saved, unit_grad):
    first_pre, first_act, second_pre, second_act, embedding, inv_norm = saved
    along = jnp.sum(embedding * unit_grad, axis=1, keepdims=True)
    embed_grad = (inv_norm * unit_grad - inv_norm * inv_norm * inv_norm * embedding * along).astype(
        jnp.bfloat16
    )
    third_grad = contract_rows(second_act, embed_grad)
    second_slope = (contract_cols(embed_grad, third) * silu_slope(second_pre)).astype(jnp.bfloat16)
    second_grad = contract_rows(first_act, second_slope)
    first_slope = (contract_cols(second_slope, second) * silu_slope(first_pre)).astype(jnp.bfloat16)
    first_grad = contract_rows(features, first_slope)
    return (first_grad, second_grad, third_grad)


class Links:
    def __init__(self, send_sems, recv_sems, size):
        self.send_sems, self.recv_sems, self.size = send_sems, recv_sems, size
        self.used = 0
        self.started = []

    def copy(self, src, dst, device):
        at = self.used
        self.used += 1
        assert at < self.size
        made = pltpu.make_async_remote_copy(
            src_ref=src,
            dst_ref=dst,
            send_sem=self.send_sems.at[at],
            recv_sem=self.recv_sems.at[at],
            device_id=device,
            device_id_type=MESH,
        )
        made.start()
        self.started.append(made)
        return made

    def finish(self):
        for made in self.started:
            made.wait_send()


def add_rows(out, terms, rows, step):
    def body(i, carry):
        at = pl.ds(pl.multiple_of(i * step, step), step)
        total = terms[0][at].astype(F32)
        for term in terms[1:]:
            total = total + term[at].astype(F32)
        out[at] = total.astype(out.dtype)
        return carry

    if rows == step:
        body(0, 0)
    else:
        lax.fori_loop(0, rows // step, body, 0)


class Ring4:
    def __init__(self, links, axis, cut, rows, land, step):
        self.links, self.axis, self.cut, self.rows, self.step = links, axis, cut, rows, step
        self.early_up, self.early_down, self.from_down, self.from_up = land
        me = lax.axis_index(axis)
        self.me = me
        self.up, self.down, self.far = lax.rem(me + 1, 4), lax.rem(me + 3, 4), lax.rem(me + 2, 4)

    def start(self):
        half = self.rows // 2
        low, high = pl.ds(0, half), pl.ds(half, half)
        up, down = {self.axis: self.up}, {self.axis: self.down}
        far = self.cut(self.far)
        self.a = self.links.copy(far.at[low], self.early_up, up)
        self.b = self.links.copy(far.at[high], self.early_down, down)
        self.c = self.links.copy(self.cut(self.up).at[high], self.from_down.at[high], up)
        self.d = self.links.copy(self.cut(self.down).at[low], self.from_up.at[low], down)

    def relay(self):
        half = self.rows // 2
        low, high = pl.ds(0, half), pl.ds(half, half)
        up, down = {self.axis: self.up}, {self.axis: self.down}
        self.a.wait_recv()
        mine = self.cut(self.up).at[low]
        add_rows(self.early_up, (mine, self.early_up), half, self.step)
        self.e = self.links.copy(self.early_up, self.from_down.at[low], up)
        self.b.wait_recv()
        mine = self.cut(self.down).at[high]
        add_rows(self.early_down, (mine, self.early_down), half, self.step)
        self.f = self.links.copy(self.early_down, self.from_up.at[high], down)

    def end(self, out):
        for made in (self.c, self.d, self.e, self.f):
            made.wait_recv()
        add_rows(out, (self.cut(self.me), self.from_down, self.from_up), self.rows, self.step)


class Direct:
    def __init__(self, links, axis, size, slots):
        self.links, self.axis, self.size, self.slots = links, axis, size, slots
        self.me = lax.axis_index(axis)

    def start(self, cut):
        self.made = []
        for k in range(1, self.size):
            to = lax.rem(self.me + k, self.size)
            self.made.append(self.links.copy(cut(to), self.slots.at[self.me], {self.axis: to}))

    def wait(self):
        for made in self.made:
            made.wait_recv()


def greet_neighbours():
    y, z, x, c = (lax.axis_index(a) for a in (AX_Y, AX_Z, AX_X, AX_C))
    barrier = pltpu.get_barrier_semaphore()
    peers = [{AX_Y: lax.rem(y + k, 4)} for k in range(1, 4)]
    peers += [{AX_Z: lax.rem(z + k, 8)} for k in range(1, 8)]
    for k in range(1, 8):
        other = lax.rem(x * 2 + c + k, 8)
        peers.append({AX_X: other // 2, AX_C: lax.rem(other, 2)})
    for peer in peers:
        pl.semaphore_signal(barrier, inc=1, device_id=peer, device_id_type=MESH)
    return barrier, len(peers)


def multiple(index, size):
    return pl.multiple_of(index * size, size)


def reduce_gradients(links, g_first, g_second, g_third, loss_tile, outs, bufs):
    (o_first, o_second, o_third, o_loss) = outs
    y, z, x, c = (lax.axis_index(a) for a in (AX_Y, AX_Z, AX_X, AX_C))
    other = {AX_C: 1 - c}
    mate = 1 - c

    a_first, a_second, a_third = bufs["a_first"], bufs["a_second"], bufs["a_third"]
    pair = [
        links.copy(g_first.at[mate], a_first, other),
        links.copy(g_second.at[mate], a_second, other),
        links.copy(g_third.at[mate], a_third, other),
    ]
    first_x = Ring4(
        links, AX_X, lambda j: a_first.at[:, pl.ds(multiple(j, 256), 256)], 512, bufs["fx"], 64
    )
    second_y = Ring4(
        links, AX_Y, lambda j: a_second.at[pl.ds(multiple(j, 256), 256)], 256, bufs["sy"], 32
    )
    pair[0].wait_recv()
    add_rows(a_first, (a_first, g_first.at[c]), 512, 16)
    first_x.start()
    pair[1].wait_recv()
    add_rows(a_second, (a_second, g_second.at[c]), 1024, 32)
    second_y.start()
    pair[2].wait_recv()
    for i in range(4):
        add_rows(a_third.at[i], (a_third.at[i], g_third.at[c, i]), 8, 1)
    third_z = Direct(links, AX_Z, 8, bufs["tz"])
    third_z.start(lambda j: a_third.at[:, j])

    first_x.relay()
    second_y.relay()

    third_z.wait()
    tz, t_sum = bufs["tz"], bufs["t_sum"]
    for i in range(4):
        tz[z, i] = a_third[i, z]
    for i in range(4):
        total = tz[0, i].astype(F32)
        for j in range(1, 8):
            total = total + tz[j, i].astype(F32)
        t_sum[i] = total.astype(BF16)
    third_y = Direct(links, AX_Y, 4, bufs["ty"])
    third_y.start(lambda j: t_sum.at[j])

    fx_sum, sy_sum = bufs["fx_sum"], bufs["sy_sum"]
    first_x.end(fx_sum)
    first_y = Ring4(
        links, AX_Y, lambda j: fx_sum.at[pl.ds(multiple(j, 128), 128)], 128, bufs["fy"], 64
    )
    first_y.start()
    second_y.end(sy_sum)
    second_x = Ring4(
        links, AX_X, lambda j: sy_sum.at[:, pl.ds(multiple(j, 128), 128)], 256, bufs["sx"], 128
    )
    second_x.start()

    third_y.wait()
    ty, ty_sum = bufs["ty"], bufs["ty_sum"]
    ty[y] = t_sum[y]
    total = ty[0].astype(F32)
    for j in range(1, 4):
        total = total + ty[j].astype(F32)
    ty_sum[...] = total.astype(BF16)
    third_x = Direct(links, AX_X, 4, bufs["tx"])
    third_x.start(lambda j: ty_sum)

    first_y.relay()
    second_x.relay()
    fy_sum, sx_sum = bufs["fy_sum"], bufs["sx_sum"]
    first_y.end(fy_sum)
    first_z = Direct(links, AX_Z, 8, bufs["fz"])
    first_z.start(lambda j: fy_sum.at[pl.ds(multiple(j, 16), 16)])
    second_x.end(sx_sum)
    second_z = Direct(links, AX_Z, 8, bufs["sz"])
    second_z.start(lambda j: sx_sum.at[pl.ds(multiple(j, 32), 32)])

    third_x.wait()
    tx = bufs["tx"]
    tx[x] = ty_sum[...]
    t_final = tx[0].astype(F32)
    for j in range(1, 4):
        t_final = t_final + tx[j].astype(F32)

    first_z.wait()
    f_final = fy_sum[pl.ds(multiple(z, 16), 16), :].astype(F32)
    fz, sz = bufs["fz"], bufs["sz"]
    fz[z] = fy_sum[pl.ds(multiple(z, 16), 16), :]
    f_final = fz[0].astype(F32)
    for j in range(1, 8):
        f_final = f_final + fz[j].astype(F32)
    second_z.wait()
    sz[z] = sx_sum[pl.ds(multiple(z, 32), 32), :]
    s_final = sz[0].astype(F32)
    for j in range(1, 8):
        s_final = s_final + sz[j].astype(F32)

    squares = jnp.sum((f_final * f_final).reshape(2, 8, 2, 128), axis=(0, 2))
    squares += jnp.sum((s_final * s_final).reshape(4, 8, 128), axis=0)
    squares += jnp.sum((t_final * t_final).reshape(2, 8, 2, 128), axis=(0, 2)) * 0.25
    f_own, s_own, t_own = bufs["f_own"], bufs["s_own"], bufs["t_own"]
    c_in, c_out, y_in, y_out, z_in, z_out = (
        bufs[k] for k in ("c_in", "c_out", "y_in", "y_out", "z_in", "z_out")
    )
    c_out[0] = squares
    c_out[1] = loss_tile[...]
    f_own[...] = f_final
    s_own[...] = s_final
    t_own[...] = t_final
    me = x * 2 + c
    others = []
    for k in range(1, 8):
        to = lax.rem(me + k, 8)
        others.append({AX_X: to // 2, AX_C: lax.rem(to, 2)})
    scalars = [links.copy(c_out, c_in.at[me], peer) for peer in others]
    ag_first, ag_second, ag_third = bufs["ag_first"], bufs["ag_second"], bufs["ag_third"]
    f_cols = pl.ds(multiple(x, 256), 256)
    s_cols = pl.ds(multiple(x, 128), 128)
    pieces = [links.copy(t_own, ag_third.at[c], other)]
    for peer in others:
        pieces.append(links.copy(f_own, ag_first.at[c, :, f_cols], peer))
        pieces.append(links.copy(s_own, ag_second.at[c, :, s_cols], peer))
    c_in[me] = c_out[...]
    ag_first[c, :, f_cols] = f_final
    ag_second[c, :, s_cols] = s_final
    ag_third[c] = t_final
    for made in scalars:
        made.wait_recv()
    total = c_in[0]
    for j in range(1, 8):
        total = total + c_in[j]
    y_out[...] = total
    y_in[y] = total
    along_y = Direct(links, AX_Y, 4, y_in)
    along_y.start(lambda j: y_out)
    along_y.wait()
    total = y_in[0]
    for j in range(1, 4):
        total = total + y_in[j]
    z_out[...] = total
    z_in[z] = total
    along_z = Direct(links, AX_Z, 8, z_in)
    along_z.start(lambda j: z_out)
    along_z.wait()
    total = z_in[0]
    for j in range(1, 8):
        total = total + z_in[j]
    norm = jnp.sqrt(jnp.sum(total[0], keepdims=True))
    factor = clip_norm / jnp.maximum(norm, clip_norm)
    o_loss[...] = jnp.broadcast_to(jnp.sum(total[1], keepdims=True), (8, 128))
    for made in pieces:
        made.wait_recv()
    for t in range(2):
        o_first[t] = ag_first[t] * factor
        o_second[t] = ag_second[t] * factor
        o_third[t] = ag_third[t] * factor


LINKS = 120


def ring_land(rows, cols):
    half = pltpu.VMEM((rows // 2, cols), BF16)
    whole = pltpu.VMEM((rows, cols), BF16)
    return (half, half, whole, whole)


GRAD_BUFS = {
    "a_first": pltpu.VMEM((512, 1024), BF16),
    "a_second": pltpu.VMEM((1024, 512), BF16),
    "a_third": pltpu.VMEM((4, 8, 16, 256), BF16),
    "fx": ring_land(512, 256),
    "sy": ring_land(256, 512),
    "tz": pltpu.VMEM((8, 4, 16, 256), BF16),
    "t_sum": pltpu.VMEM((4, 16, 256), BF16),
    "ty": pltpu.VMEM((4, 16, 256), BF16),
    "ty_sum": pltpu.VMEM((16, 256), BF16),
    "tx": pltpu.VMEM((4, 16, 256), BF16),
    "fx_sum": pltpu.VMEM((512, 256), BF16),
    "sy_sum": pltpu.VMEM((256, 512), BF16),
    "fy": ring_land(128, 256),
    "sx": ring_land(256, 128),
    "fy_sum": pltpu.VMEM((128, 256), BF16),
    "sx_sum": pltpu.VMEM((256, 128), BF16),
    "fz": pltpu.VMEM((8, 16, 256), BF16),
    "sz": pltpu.VMEM((8, 32, 128), BF16),
    "f_own": pltpu.VMEM((16, 256), F32),
    "s_own": pltpu.VMEM((32, 128), F32),
    "t_own": pltpu.VMEM((16, 256), F32),
    "c_in": pltpu.VMEM((8, 2, 8, 128), F32),
    "c_out": pltpu.VMEM((2, 8, 128), F32),
    "y_in": pltpu.VMEM((4, 2, 8, 128), F32),
    "y_out": pltpu.VMEM((2, 8, 128), F32),
    "z_in": pltpu.VMEM((8, 2, 8, 128), F32),
    "z_out": pltpu.VMEM((2, 8, 128), F32),
    "ag_first": pltpu.VMEM((2, 16, 1024), F32),
    "ag_second": pltpu.VMEM((2, 32, 512), F32),
    "ag_third": pltpu.VMEM((2, 16, 256), F32),
}


def gradient_kernel(g_first, g_second, g_third, loss, o_first, o_second, o_third, o_loss, bufs, send, recv):
    barrier, peers = greet_neighbours()
    pl.semaphore_wait(barrier, peers)
    links = Links(send, recv, LINKS)
    outs = (o_first, o_second, o_third, o_loss)
    reduce_gradients(links, g_first, g_second, g_third, loss, outs, bufs)
    links.finish()


def reduced_gradients(g_first, g_second, g_third, loss):
    vmem = pl.BlockSpec(memory_space=pltpu.VMEM)
    return pl.pallas_call(
        gradient_kernel,
        out_shape=(
            jax.ShapeDtypeStruct((2, 16, 1024), F32),
            jax.ShapeDtypeStruct((2, 32, 512), F32),
            jax.ShapeDtypeStruct((2, 16, 256), F32),
            jax.ShapeDtypeStruct((8, 128), F32),
        ),
        in_specs=[vmem] * 4,
        out_specs=(vmem,) * 4,
        scratch_shapes=[
            GRAD_BUFS,
            pltpu.SemaphoreType.DMA((LINKS,)),
            pltpu.SemaphoreType.DMA((LINKS,)),
        ],
        compiler_params=pltpu.CompilerParams(
            collective_id=0, has_side_effects=True, vmem_limit_bytes=60 * 1024 * 1024
        ),
        name="reduce_gradients",
    )(g_first, g_second, g_third, loss)


def per_device(
    query_features,
    positive_features,
    negative_features,
    positive_ids,
    positive_counts,
    negative_ids,
    negative_counts,
    query_first,
    query_second,
    query_third,
    item_first,
    item_second,
    item_third,
):
    own_rows = query_features.shape[0]
    query_saved, query_unit = tower_forward(query_features, query_first, query_second, query_third)
    item_features = jnp.concatenate([positive_features, negative_features], axis=0)
    item_saved, item_unit = tower_forward(item_features, item_first, item_second, item_third)
    positive_unit = item_unit[:own_rows]
    negative_unit = item_unit[own_rows:]
    group_unit = collect(query_unit, NEG, 0)
    shard_unit = collect(negative_unit, DP, 0)
    scores = (
        contract_cols(group_unit, shard_unit) * inv_temp
        - jnp.log(negative_counts.astype(jnp.float32))[None, :]
    )
    weights = jnp.where(positive_ids[:, None] != negative_ids[None, :], jnp.exp(scores), 0.0)
    positive_logit = jnp.sum(
        query_unit.astype(jnp.float32) * positive_unit.astype(jnp.float32), axis=1
    ) * inv_temp - jnp.log(positive_counts.astype(jnp.float32))
    positive_exp = jnp.exp(positive_logit)
    offset = lax.axis_index(NEG) * own_rows
    partial_value = jnp.sum(weights, axis=1)
    own_part = lax.dynamic_slice(partial_value, (offset,), (own_rows,)) + positive_exp
    partial_value = lax.dynamic_update_slice(partial_value, own_part, (offset,))
    denom = over_copies(partial_value, NEG)
    own_denom = lax.dynamic_slice(denom, (offset,), (own_rows,))
    loss_part = jnp.sum(jnp.log(own_denom) - positive_logit)
    softmax_weights = (weights / denom[:, None]).astype(jnp.bfloat16)
    positive_slope = positive_exp / own_denom - 1.0
    block = softmax_weights
    query_sum = sent_and_summed(
        jnp.dot(block, shard_unit, preferred_element_type=jnp.float32), NEG, 0
    )
    query_grad = (
        query_sum + positive_slope[:, None] * positive_unit.astype(jnp.float32)
    ) * inv_temp
    block = softmax_weights
    negative_sum = own_rows_2(contract_rows(block, group_unit), DP)
    positive_grad = positive_slope[:, None] * query_unit.astype(jnp.float32) * inv_temp
    item_grad = jnp.concatenate([positive_grad, negative_sum * inv_temp], axis=0)
    query_grads = tower_backward(query_features, query_second, query_third, query_saved, query_grad)
    item_grads = tower_backward(item_features, item_second, item_third, item_saved, item_grad)
    stacked = [
        jnp.stack([a.astype(BF16), b.astype(BF16)]) for a, b in zip(query_grads, item_grads)
    ]
    loss_tile = jnp.broadcast_to(loss_part * (1.0 / 1024.0), (8, 128))
    first, second, third, loss = reduced_gradients(
        stacked[0], stacked[1], stacked[2].reshape(2, 4, 8, 16, 256), loss_tile
    )
    mean_loss = loss[0, 0] / (own_rows * lax.axis_size(DP) * lax.axis_size(NEG))
    return (mean_loss, first[0], second[0], third[0], first[1], second[1], third[1])


def solution(mesh):
    torus = Mesh(mesh.devices.reshape(4, 8, 4, 2), ("dp_0", "dp_1", "neg_0", "neg_1"))
    placed = (
        P(DP_NEG, None),
        P(DP_NEG, None),
        P(NEG_DP, None),
        P(DP),
        P(DP_NEG),
        P(NEG),
        P(NEG),
        P(),
        P(),
        P(),
        P(),
        P(),
        P(),
    )
    return jax.shard_map(
        per_device,
        mesh=torus,
        in_specs=placed,
        out_specs=(
            P(),
            P(DP, None),
            P(DP, None),
            P(DP, None),
            P(DP, None),
            P(DP, None),
            P(DP, None),
        ),
        check_vma=False,
    )
```

```python
import jax
import jax.numpy as jnp
from jax import lax
from jax.experimental import pallas as pl
from jax.experimental.pallas import tpu as pltpu
from jax.sharding import Mesh
from jax.sharding import PartitionSpec as P

NEG = ("neg_0", "neg_1")
DP = ("dp_0", "dp_1")
DP_NEG = ("dp_0", "dp_1", "neg_0", "neg_1")
NEG_DP = ("neg_0", "neg_1", "dp_0", "dp_1")
AX_Y, AX_Z, AX_X, AX_C = "dp_0", "dp_1", "neg_0", "neg_1"
MESH = pl.DeviceIdType.MESH
F32 = jnp.float32
BF16 = jnp.bfloat16

inv_temp = 20.0
clip_norm = 256.0
LOG2_E = 1.4426950408889634


class Links:
    def __init__(self, send_sems, recv_sems, size):
        self.send_sems, self.recv_sems, self.size = send_sems, recv_sems, size
        self.used = 0
        self.started = []

    def copy(self, src, dst, device):
        at = self.used
        self.used += 1
        assert at < self.size
        made = pltpu.make_async_remote_copy(
            src_ref=src,
            dst_ref=dst,
            send_sem=self.send_sems.at[at],
            recv_sem=self.recv_sems.at[at],
            device_id=device,
            device_id_type=MESH,
        )
        made.start()
        self.started.append(made)
        return made

    def finish(self):
        for made in self.started:
            made.wait_send()


def add_rows(out, terms, rows, step):
    def body(i, carry):
        at = pl.ds(pl.multiple_of(i * step, step), step)
        total = terms[0][at].astype(F32)
        for term in terms[1:]:
            total = total + term[at].astype(F32)
        out[at] = total.astype(out.dtype)
        return carry

    if rows == step:
        body(0, 0)
    else:
        lax.fori_loop(0, rows // step, body, 0)


class Ring4:
    def __init__(self, links, axis, cut, rows, land, step):
        self.links, self.axis, self.cut, self.rows, self.step = links, axis, cut, rows, step
        self.early_up, self.early_down, self.from_down, self.from_up = land
        me = lax.axis_index(axis)
        self.me = me
        self.up, self.down, self.far = lax.rem(me + 1, 4), lax.rem(me + 3, 4), lax.rem(me + 2, 4)

    def start(self):
        half = self.rows // 2
        low, high = pl.ds(0, half), pl.ds(half, half)
        up, down = {self.axis: self.up}, {self.axis: self.down}
        far = self.cut(self.far)
        self.a = self.links.copy(far.at[low], self.early_up, up)
        self.b = self.links.copy(far.at[high], self.early_down, down)
        self.c = self.links.copy(self.cut(self.up).at[high], self.from_down.at[high], up)
        self.d = self.links.copy(self.cut(self.down).at[low], self.from_up.at[low], down)

    def relay(self):
        half = self.rows // 2
        low, high = pl.ds(0, half), pl.ds(half, half)
        up, down = {self.axis: self.up}, {self.axis: self.down}
        self.a.wait_recv()
        mine = self.cut(self.up).at[low]
        add_rows(self.early_up, (mine, self.early_up), half, self.step)
        self.e = self.links.copy(self.early_up, self.from_down.at[low], up)
        self.b.wait_recv()
        mine = self.cut(self.down).at[high]
        add_rows(self.early_down, (mine, self.early_down), half, self.step)
        self.f = self.links.copy(self.early_down, self.from_up.at[high], down)

    def end(self, out):
        for made in (self.c, self.d, self.e, self.f):
            made.wait_recv()
        add_rows(out, (self.cut(self.me), self.from_down, self.from_up), self.rows, self.step)


class Direct:
    def __init__(self, links, axis, size, slots):
        self.links, self.axis, self.size, self.slots = links, axis, size, slots
        self.me = lax.axis_index(axis)

    def start(self, cut):
        self.made = []
        for k in range(1, self.size):
            to = lax.rem(self.me + k, self.size)
            self.made.append(self.links.copy(cut(to), self.slots.at[self.me], {self.axis: to}))

    def wait(self):
        for made in self.made:
            made.wait_recv()


def greet_neighbours():
    y, z, x, c = (lax.axis_index(a) for a in (AX_Y, AX_Z, AX_X, AX_C))
    barrier = pltpu.get_barrier_semaphore()
    peers = [{AX_Y: lax.rem(y + k, 4)} for k in range(1, 4)]
    peers += [{AX_Z: lax.rem(z + k, 8)} for k in range(1, 8)]
    for k in range(1, 8):
        other = lax.rem(x * 2 + c + k, 8)
        peers.append({AX_X: other // 2, AX_C: lax.rem(other, 2)})
    for peer in peers:
        pl.semaphore_signal(barrier, inc=1, device_id=peer, device_id_type=MESH)
    return barrier, len(peers)


def multiple(index, size):
    return pl.multiple_of(index * size, size)


def reduce_gradients(links, g_first, g_second, g_third, loss_tile, outs, bufs):
    (o_first, o_second, o_third, o_loss) = outs
    y, z, x, c = (lax.axis_index(a) for a in (AX_Y, AX_Z, AX_X, AX_C))
    other = {AX_C: 1 - c}
    mate = 1 - c

    a_first, a_second, a_third = bufs["a_first"], bufs["a_second"], bufs["a_third"]
    pair = [
        links.copy(g_first.at[mate], a_first, other),
        links.copy(g_second.at[mate], a_second, other),
        links.copy(g_third.at[mate], a_third, other),
    ]
    first_x = Ring4(
        links, AX_X, lambda j: a_first.at[:, pl.ds(multiple(j, 256), 256)], 512, bufs["fx"], 64
    )
    second_y = Ring4(
        links, AX_Y, lambda j: a_second.at[pl.ds(multiple(j, 256), 256)], 256, bufs["sy"], 32
    )
    pair[0].wait_recv()
    add_rows(a_first, (a_first, g_first.at[c]), 512, 16)
    first_x.start()
    pair[1].wait_recv()
    add_rows(a_second, (a_second, g_second.at[c]), 1024, 32)
    second_y.start()
    pair[2].wait_recv()
    for i in range(4):
        add_rows(a_third.at[i], (a_third.at[i], g_third.at[c, i]), 8, 1)
    third_z = Direct(links, AX_Z, 8, bufs["tz"])
    third_z.start(lambda j: a_third.at[:, j])

    first_x.relay()
    second_y.relay()

    third_z.wait()
    tz, t_sum = bufs["tz"], bufs["t_sum"]
    for i in range(4):
        tz[z, i] = a_third[i, z]
    for i in range(4):
        total = tz[0, i].astype(F32)
        for j in range(1, 8):
            total = total + tz[j, i].astype(F32)
        t_sum[i] = total.astype(BF16)
    third_y = Direct(links, AX_Y, 4, bufs["ty"])
    third_y.start(lambda j: t_sum.at[j])

    fx_sum, sy_sum = bufs["fx_sum"], bufs["sy_sum"]
    first_x.end(fx_sum)
    first_y = Ring4(
        links, AX_Y, lambda j: fx_sum.at[pl.ds(multiple(j, 128), 128)], 128, bufs["fy"], 64
    )
    first_y.start()
    second_y.end(sy_sum)
    second_x = Ring4(
        links, AX_X, lambda j: sy_sum.at[:, pl.ds(multiple(j, 128), 128)], 256, bufs["sx"], 128
    )
    second_x.start()

    third_y.wait()
    ty, ty_sum = bufs["ty"], bufs["ty_sum"]
    ty[y] = t_sum[y]
    total = ty[0].astype(F32)
    for j in range(1, 4):
        total = total + ty[j].astype(F32)
    ty_sum[...] = total.astype(BF16)
    third_x = Direct(links, AX_X, 4, bufs["tx"])
    third_x.start(lambda j: ty_sum)

    first_y.relay()
    second_x.relay()
    fy_sum, sx_sum = bufs["fy_sum"], bufs["sx_sum"]
    first_y.end(fy_sum)
    first_z = Direct(links, AX_Z, 8, bufs["fz"])
    first_z.start(lambda j: fy_sum.at[pl.ds(multiple(j, 16), 16)])
    second_x.end(sx_sum)
    second_z = Direct(links, AX_Z, 8, bufs["sz"])
    second_z.start(lambda j: sx_sum.at[pl.ds(multiple(j, 32), 32)])

    third_x.wait()
    tx = bufs["tx"]
    tx[x] = ty_sum[...]
    t_final = tx[0].astype(F32)
    for j in range(1, 4):
        t_final = t_final + tx[j].astype(F32)

    first_z.wait()
    f_final = fy_sum[pl.ds(multiple(z, 16), 16), :].astype(F32)
    fz, sz = bufs["fz"], bufs["sz"]
    fz[z] = fy_sum[pl.ds(multiple(z, 16), 16), :]
    f_final = fz[0].astype(F32)
    for j in range(1, 8):
        f_final = f_final + fz[j].astype(F32)
    second_z.wait()
    sz[z] = sx_sum[pl.ds(multiple(z, 32), 32), :]
    s_final = sz[0].astype(F32)
    for j in range(1, 8):
        s_final = s_final + sz[j].astype(F32)

    squares = jnp.sum((f_final * f_final).reshape(2, 8, 2, 128), axis=(0, 2))
    squares += jnp.sum((s_final * s_final).reshape(4, 8, 128), axis=0)
    squares += jnp.sum((t_final * t_final).reshape(2, 8, 2, 128), axis=(0, 2)) * 0.25
    f_own, s_own, t_own = bufs["f_own"], bufs["s_own"], bufs["t_own"]
    c_in, c_out, y_in, y_out, z_in, z_out = (
        bufs[k] for k in ("c_in", "c_out", "y_in", "y_out", "z_in", "z_out")
    )
    c_out[0] = squares
    c_out[1] = loss_tile
    f_own[...] = f_final
    s_own[...] = s_final
    t_own[...] = t_final
    me = x * 2 + c
    others = []
    for k in range(1, 8):
        to = lax.rem(me + k, 8)
        others.append({AX_X: to // 2, AX_C: lax.rem(to, 2)})
    scalars = [links.copy(c_out, c_in.at[me], peer) for peer in others]
    ag_first, ag_second, ag_third = bufs["ag_first"], bufs["ag_second"], bufs["ag_third"]
    f_cols = pl.ds(multiple(x, 256), 256)
    s_cols = pl.ds(multiple(x, 128), 128)
    pieces = [links.copy(t_own, ag_third.at[c], other)]
    for peer in others:
        pieces.append(links.copy(f_own, ag_first.at[c, :, f_cols], peer))
        pieces.append(links.copy(s_own, ag_second.at[c, :, s_cols], peer))
    c_in[me] = c_out[...]
    ag_first[c, :, f_cols] = f_final
    ag_second[c, :, s_cols] = s_final
    ag_third[c] = t_final
    for made in scalars:
        made.wait_recv()
    total = c_in[0]
    for j in range(1, 8):
        total = total + c_in[j]
    y_out[...] = total
    y_in[y] = total
    along_y = Direct(links, AX_Y, 4, y_in)
    along_y.start(lambda j: y_out)
    along_y.wait()
    total = y_in[0]
    for j in range(1, 4):
        total = total + y_in[j]
    z_out[...] = total
    z_in[z] = total
    along_z = Direct(links, AX_Z, 8, z_in)
    along_z.start(lambda j: z_out)
    along_z.wait()
    total = z_in[0]
    for j in range(1, 8):
        total = total + z_in[j]
    norm = jnp.sqrt(jnp.sum(total[0], keepdims=True))
    factor = clip_norm / jnp.maximum(norm, clip_norm)
    o_loss[...] = jnp.broadcast_to(jnp.sum(total[1], keepdims=True), (8, 128))
    for made in pieces:
        made.wait_recv()
    for t in range(2):
        o_first[t] = ag_first[t] * factor
        o_second[t] = ag_second[t] * factor
        o_third[t] = ag_third[t] * factor


LINKS = 192


def ring_land(rows, cols):
    half = pltpu.VMEM((rows // 2, cols), BF16)
    whole = pltpu.VMEM((rows, cols), BF16)
    return (half, half, whole, whole)


GRAD_BUFS = {
    "a_first": pltpu.VMEM((512, 1024), BF16),
    "a_second": pltpu.VMEM((1024, 512), BF16),
    "a_third": pltpu.VMEM((4, 8, 16, 256), BF16),
    "fx": ring_land(512, 256),
    "sy": ring_land(256, 512),
    "tz": pltpu.VMEM((8, 4, 16, 256), BF16),
    "t_sum": pltpu.VMEM((4, 16, 256), BF16),
    "ty": pltpu.VMEM((4, 16, 256), BF16),
    "ty_sum": pltpu.VMEM((16, 256), BF16),
    "tx": pltpu.VMEM((4, 16, 256), BF16),
    "fx_sum": pltpu.VMEM((512, 256), BF16),
    "sy_sum": pltpu.VMEM((256, 512), BF16),
    "fy": ring_land(128, 256),
    "sx": ring_land(256, 128),
    "fy_sum": pltpu.VMEM((128, 256), BF16),
    "sx_sum": pltpu.VMEM((256, 128), BF16),
    "fz": pltpu.VMEM((8, 16, 256), BF16),
    "sz": pltpu.VMEM((8, 32, 128), BF16),
    "f_own": pltpu.VMEM((16, 256), F32),
    "s_own": pltpu.VMEM((32, 128), F32),
    "t_own": pltpu.VMEM((16, 256), F32),
    "c_in": pltpu.VMEM((8, 2, 8, 128), F32),
    "c_out": pltpu.VMEM((2, 8, 128), F32),
    "y_in": pltpu.VMEM((4, 2, 8, 128), F32),
    "y_out": pltpu.VMEM((2, 8, 128), F32),
    "z_in": pltpu.VMEM((8, 2, 8, 128), F32),
    "z_out": pltpu.VMEM((2, 8, 128), F32),
    "ag_first": pltpu.VMEM((2, 16, 1024), F32),
    "ag_second": pltpu.VMEM((2, 32, 512), F32),
    "ag_third": pltpu.VMEM((2, 16, 256), F32),
}


Q_ROWS, P_ROWS, N_ROWS = pl.ds(0, 256), pl.ds(256, 256), pl.ds(512, 128)
I_ROWS = pl.ds(256, 384)

STEP_BUFS = {
    "w1": pltpu.VMEM((2, 512, 1024), BF16),
    "w2": pltpu.VMEM((2, 1024, 512), BF16),
    "w3": pltpu.VMEM((2, 512, 256), BF16),
    "x": pltpu.VMEM((640, 512), BF16),
    "a1": pltpu.VMEM((640, 1024), BF16),
    "a2": pltpu.VMEM((640, 512), BF16),
    "s1": pltpu.VMEM((640, 1024), F32),
    "s2": pltpu.VMEM((640, 512), F32),
    "emb": pltpu.VMEM((640, 256), F32),
    "inv": pltpu.VMEM((640, 1), F32),
    "eg": pltpu.VMEM((640, 256), BF16),
    "d2": pltpu.VMEM((640, 512), BF16),
    "d1": pltpu.VMEM((640, 1024), BF16),
    "xt": pltpu.VMEM((512, 640), BF16),
    "a1t": pltpu.VMEM((1024, 640), BF16),
    "a2t": pltpu.VMEM((512, 640), BF16),
    "eye": pltpu.VMEM((256, 256), BF16),
    "pos": pltpu.VMEM((256, 256), BF16),
    "q": pltpu.VMEM((2048, 256), BF16),
    "qs": pltpu.VMEM((2048, 256), BF16),
    "n": pltpu.VMEM((2048, 256), BF16),
    "nt": pltpu.VMEM((256, 2048), BF16),
    "et": pltpu.VMEM((2048, 2048), BF16),
    "turn": pltpu.VMEM((128, 128), F32),
    "ids": pltpu.VMEM((2048, 128), F32),
    "log": pltpu.VMEM((2048, 128), F32),
    "part": pltpu.VMEM((8, 2048), F32),
    "den_out": pltpu.VMEM((16, 128), F32),
    "den_in": pltpu.VMEM((8, 16, 128), F32),
    "den": pltpu.VMEM((16, 128), F32),
    "p_out": pltpu.VMEM((2, 4, 256, 256), BF16),
    "p_pair": pltpu.VMEM((4, 256, 256), BF16),
    "p_ring": ring_land(256, 256),
    "p_sum": pltpu.VMEM((256, 256), F32),
    "g_out": pltpu.VMEM((2048, 256), BF16),
    "g_ring": ring_land(512, 256),
    "g_sum": pltpu.VMEM((512, 256), BF16),
    "g_z": pltpu.VMEM((8, 64, 256), BF16),
    "g_first": pltpu.VMEM((2, 512, 1024), BF16),
    "g_second": pltpu.VMEM((2, 1024, 512), BF16),
    "g_third": pltpu.VMEM((2, 4, 8, 16, 256), BF16),
}


def dot(a, b):
    return jnp.dot(a, b, preferred_element_type=F32)


def dot_cols(a, b):
    return lax.dot_general(a, b, (((1,), (1,)), ((), ())), preferred_element_type=F32)


def silu_both(pre):
    sigma = 0.5 * jnp.tanh(0.5 * pre) + 0.5
    act = pre * sigma
    return act, sigma * (1.0 + pre - act)


def forward(b, t, rows):
    def layer(i, carry):
        cols = pl.ds(multiple(i, 512), 512)
        act, slope = silu_both(dot(b["x"][rows, :], b["w1"][t, :, cols]))
        b["a1"][rows, cols] = act.astype(BF16)
        b["s1"][rows, cols] = slope
        return carry

    lax.fori_loop(0, 2, layer, 0)
    act, slope = silu_both(dot(b["a1"][rows, :], b["w2"][t]))
    b["a2"][rows, :] = act.astype(BF16)
    b["s2"][rows, :] = slope
    embedding = dot(b["a2"][rows, :], b["w3"][t])
    inv_norm = lax.rsqrt(jnp.sum(embedding * embedding, axis=1, keepdims=True) + 1.0)
    b["emb"][rows, :] = embedding
    b["inv"][rows, :] = inv_norm
    return (embedding * inv_norm).astype(BF16)


def backward(b, t, rows, unit_grad):
    embedding, inv_norm = b["emb"][rows, :], b["inv"][rows, :]
    along = jnp.sum(embedding * unit_grad, axis=1, keepdims=True)
    embed_grad = inv_norm * unit_grad - inv_norm * inv_norm * inv_norm * embedding * along
    b["eg"][rows, :] = embed_grad.astype(BF16)
    slope = dot_cols(b["eg"][rows, :], b["w3"][t]) * b["s2"][rows, :]
    b["d2"][rows, :] = slope.astype(BF16)

    def layer(i, carry):
        cols = pl.ds(multiple(i, 512), 512)
        slope = dot_cols(b["d2"][rows, :], b["w2"][t, cols, :]) * b["s1"][rows, cols]
        b["d1"][rows, cols] = slope.astype(BF16)
        return carry

    lax.fori_loop(0, 2, layer, 0)


def weight_gradients(b, t, rows):
    def first(i, carry):
        cols = pl.ds(multiple(i, 512), 512)
        b["g_first"][t, :, cols] = dot(b["xt"][:, rows], b["d1"][rows, cols]).astype(BF16)
        return carry

    lax.fori_loop(0, 2, first, 0)

    def second(i, carry):
        at = pl.ds(multiple(i, 512), 512)
        b["g_second"][t, at, :] = dot(b["a1t"][at, rows], b["d2"][rows, :]).astype(BF16)
        return carry

    lax.fori_loop(0, 2, second, 0)
    third = dot(b["a2t"][:, rows], b["eg"][rows, :]).astype(BF16)
    b["g_third"][t] = third.reshape(4, 8, 16, 256)


def turn_activations(b, rows):
    for name, cols in (("x", 512), ("a1", 1024), ("a2", 512)):

        def block(i, carry, name=name):
            at = pl.ds(multiple(i, 256), 256)
            turned = dot_cols(b["eye"][...], b[name][rows, at])
            b[name + "t"][at, rows] = turned.astype(BF16)
            return carry

        lax.fori_loop(0, cols // 256, block, 0)


def column(row):
    return jnp.broadcast_to(row, (128, 128)).T


def score_group(b, pos_ids, u):
    at = pl.ds(multiple(u, 512), 512)
    for h in range(2):
        half = pl.ds(pl.multiple_of(u * 512 + h * 256, 256), 256)
        b["nt"][:, half] = dot_cols(b["eye"][...], b["n"][half, :]).astype(BF16)

    def block(i, carry):
        cols = pl.ds(multiple(i, 512), 512)
        products = dot_cols(b["n"][at, :], b["q"][cols, :])
        logs = jnp.concatenate([b["log"][at, :]] * 4, axis=1)
        ids = jnp.concatenate([b["ids"][at, :]] * 4, axis=1)
        weights = jnp.exp2(products * (inv_temp * LOG2_E) - logs)
        weights = jnp.where(pos_ids[:, cols] != ids, weights, 0.0)
        b["et"][at, cols] = weights.astype(BF16)
        b["part"][:, cols] += jnp.sum(weights.reshape(64, 8, 512), axis=0)
        return carry

    lax.fori_loop(0, 4, block, 0)


def step_kernel(
    query_x,
    positive_x,
    negative_x,
    q1,
    q2,
    q3,
    i1,
    i2,
    i3,
    pos_ids,
    pos_counts,
    neg_ids,
    neg_counts,
    o_first,
    o_second,
    o_third,
    o_loss,
    b,
    grad_bufs,
    load,
    send,
    recv,
):
    y, z, x, c = (lax.axis_index(a) for a in (AX_Y, AX_Z, AX_X, AX_C))
    me = x * 2 + c
    barrier, peers = greet_neighbours()
    links = Links(send, recv, LINKS)

    loads = [
        (negative_x, b["x"].at[pl.ds(512, 64)]),
        (i1, b["w1"].at[1]),
        (i2, b["w2"].at[1]),
        (i3, b["w3"].at[1]),
        (query_x, b["x"].at[Q_ROWS]),
        (q1, b["w1"].at[0]),
        (q2, b["w2"].at[0]),
        (q3, b["w3"].at[0]),
        (positive_x, b["x"].at[P_ROWS]),
    ]
    loads = [pltpu.make_async_copy(s, d, load.at[k]) for k, (s, d) in enumerate(loads)]
    for made in loads:
        made.start()

    b["x"][pl.ds(576, 64), :] = jnp.zeros((64, 512), BF16)
    b["part"][...] = jnp.zeros((8, 2048), F32)
    ones = lax.broadcasted_iota(jnp.int32, (256, 256), 0) == lax.broadcasted_iota(
        jnp.int32, (256, 256), 1
    )
    b["eye"][...] = jnp.where(ones, 1.0, 0.0).astype(BF16)

    for made in loads[:4]:
        made.wait()
    n = b["n"]
    unit = forward(b, 1, N_ROWS)

    def n_block(yy, zz):
        return n.at[pl.ds(pl.multiple_of((yy * 8 + zz) * 64, 64), 64)]

    def n_half(yy, zz, h):
        return n.at[pl.ds(pl.multiple_of((yy * 8 + zz) * 64 + h * 32, 32), 32)]

    n[pl.ds(pl.multiple_of((y * 8 + z) * 64, 64), 64), :] = unit[:64]
    pl.semaphore_wait(barrier, peers)
    y_up, y_down = lax.rem(y + 1, 4), lax.rem(y + 3, 4)
    order = (1, 7, 2, 6, 3, 5, 4)
    n_z, n_y = {}, {}
    for k in order:
        n_z[k] = links.copy(n_block(y, z), n_block(y, z), {AX_Z: lax.rem(z + k, 8)})

    def n_forward(k):
        zz = lax.rem(z - k + 8, 8)
        n_y[k] = (
            links.copy(n_block(y, zz), n_block(y, zz), {AX_Y: y_up}),
            links.copy(n_block(y, zz), n_block(y, zz), {AX_Y: y_down}),
        )

    n_forward(0)

    for made in loads[4:8]:
        made.wait()
    q = b["q"]
    q_own = forward(b, 0, Q_ROWS)

    def q_block(xx, cc):
        return q.at[pl.ds(pl.multiple_of((xx * 2 + cc) * 256, 256), 256)]

    def q_half(xx, cc, h):
        return q.at[pl.ds(pl.multiple_of((xx * 2 + cc) * 256 + h * 128, 128), 128)]

    q[pl.ds(multiple(me, 256), 256), :] = q_own
    x_up, x_down, x_far = lax.rem(x + 1, 4), lax.rem(x + 3, 4), lax.rem(x + 2, 4)
    other = {AX_C: 1 - c}
    q_up = links.copy(q_block(x, c), q_block(x, c), {AX_X: x_up})
    q_down = links.copy(q_block(x, c), q_block(x, c), {AX_X: x_down})
    q_pair = [links.copy(q_block(x, c), q_block(x, c), other)]

    loads[8].wait()
    b["pos"][...] = forward(b, 1, P_ROWS)

    for k in order[:4]:
        n_z[k].wait_recv()
        n_forward(k)
    q_up.wait_recv()
    q_low = links.copy(q_half(x_down, c, 0), q_half(x_down, c, 0), {AX_X: x_up})
    q_pair.append(links.copy(q_block(x_down, c), q_block(x_down, c), other))
    q_down.wait_recv()
    q_high = links.copy(q_half(x_up, c, 1), q_half(x_up, c, 1), {AX_X: x_down})
    q_pair.append(links.copy(q_block(x_up, c), q_block(x_up, c), other))
    for k in order[4:]:
        n_z[k].wait_recv()
        n_forward(k)

    turn = b["turn"]
    turn[...] = jnp.zeros((128, 128), F32)
    turn[pl.ds(0, 16), :] = neg_ids[...].astype(F32)
    turn[pl.ds(16, 16), :] = jnp.log(neg_counts[...].astype(F32)) * LOG2_E
    turned = turn[...].T
    for j in range(16):
        b["ids"][pl.ds(j * 128, 128), :] = jnp.broadcast_to(turned[:, j : j + 1], (128, 128))
        b["log"][pl.ds(j * 128, 128), :] = jnp.broadcast_to(
            turned[:, 16 + j : 17 + j], (128, 128)
        )

    def n_relay(k):
        zz = lax.rem(z - k + 8, 8)
        from_down, from_up = n_y[k]
        from_down.wait_recv()
        low = links.copy(n_half(y_down, zz, 0), n_half(y_down, zz, 0), {AX_Y: y_up})
        from_up.wait_recv()
        high = links.copy(n_half(y_up, zz, 1), n_half(y_up, zz, 1), {AX_Y: y_down})
        return (low, high)

    n_far = []
    for k in (0,) + order[:4]:
        n_far.extend(n_relay(k))
    q_low.wait_recv()
    q_pair.append(links.copy(q_half(x_far, c, 0), q_half(x_far, c, 0), other))
    q_high.wait_recv()
    q_pair.append(links.copy(q_half(x_far, c, 1), q_half(x_far, c, 1), other))
    for k in order[4:]:
        n_far.extend(n_relay(k))
    turn_activations(b, Q_ROWS)
    turn_activations(b, P_ROWS)
    turn_activations(b, N_ROWS)
    for made in q_pair:
        made.wait_recv()
    score_group(b, pos_ids, y)
    score_group(b, pos_ids, y_up)
    score_group(b, pos_ids, y_down)

    own = b["q"][pl.ds(multiple(me, 256), 256), :].astype(F32)
    along = jnp.sum(own * b["pos"][...].astype(F32), axis=1, keepdims=True)
    logits = []
    for h in range(2):
        row = jnp.broadcast_to(along[h * 128 : (h + 1) * 128], (128, 128)).T[0:1, :]
        logits.append(row * inv_temp - jnp.log(pos_counts[h : h + 1, :].astype(F32)))

    for made in n_far:
        made.wait_recv()
    score_group(b, pos_ids, lax.rem(y + 2, 4))

    den_out, den_in = b["den_out"], b["den_in"]
    for j in range(16):
        den_out[pl.ds(j, 1), :] = jnp.sum(b["part"][:, j * 128 : (j + 1) * 128], axis=0, keepdims=True)
    for h in range(2):
        at = pl.ds(me * 2 + h, 1)
        den_out[at, :] = den_out[at, :] + jnp.exp(logits[h])
    group = []
    for k in range(1, 8):
        to = lax.rem(me + k, 8)
        group.append({AX_X: to // 2, AX_C: lax.rem(to, 2)})
    sums = [links.copy(den_out, den_in.at[me], peer) for peer in group]
    den_in[me] = den_out[...]

    p_out = b["p_out"]

    def query_block(cc, i):
        cols = pl.ds(pl.multiple_of((i * 2 + cc) * 256, 256), 256)
        p_out[cc, i] = dot(b["nt"][...], b["et"][:, cols]).astype(BF16)

    def theirs(i, carry):
        query_block(1 - c, i)
        return carry

    def ours(i, carry):
        query_block(c, i)
        return carry

    lax.fori_loop(0, 4, theirs, 0)
    p_pair = b["p_pair"]
    pair = links.copy(p_out.at[1 - c], p_pair, other)
    for made in sums:
        made.wait_recv()
    total = den_in[0]
    for j in range(1, 8):
        total = total + den_in[j]
    b["den"][...] = total
    turn[pl.ds(0, 16), :] = 1.0 / total
    turned = turn[...].T
    for j in range(16):
        at = pl.ds(j * 128, 128)
        b["qs"][at, :] = (q[at, :].astype(F32) * turned[:, j : j + 1]).astype(BF16)

    g_out = b["g_out"]

    def negative_rows(u):
        at = pl.ds(multiple(u, 512), 512)
        g_out[at, :] = dot(b["et"][at, :], b["qs"][...]).astype(BF16)

    g_y = Ring4(links, AX_Y, lambda j: g_out.at[pl.ds(multiple(j, 512), 512)], 512, b["g_ring"], 64)
    negative_rows(g_y.far)
    negative_rows(g_y.up)
    negative_rows(g_y.down)
    g_y.start()
    negative_rows(g_y.me)
    lax.fori_loop(0, 4, ours, 0)
    pair.wait_recv()
    for i in range(4):
        add_rows(p_pair.at[i], (p_pair.at[i], p_out.at[c, i]), 256, 64)
    p_x = Ring4(links, AX_X, lambda j: p_pair.at[j], 256, b["p_ring"], 128)
    p_x.start()

    losses, slopes, scales = [], [], []
    for h in range(2):
        den = b["den"][pl.ds(me * 2 + h, 1), :]
        losses.append(jnp.log(den) - logits[h])
        slope = column(jnp.exp(logits[h]) / den - 1.0) * inv_temp
        slopes.append(jnp.concatenate([slope, slope], axis=1))
        scale = column(inv_temp / den)
        scales.append(jnp.concatenate([scale, scale], axis=1))
    slopes = jnp.concatenate(slopes, axis=0)
    scales = jnp.concatenate(scales, axis=0)
    loss_tile = jnp.concatenate(losses + [jnp.zeros((6, 128), F32)], axis=0)
    g_y.relay()
    own = q[pl.ds(multiple(me, 256), 256), :].astype(F32)
    backward(b, 1, P_ROWS, slopes * own)
    p_x.relay()
    g_sum = b["g_sum"]
    g_y.end(g_sum)
    g_z = Direct(links, AX_Z, 8, b["g_z"])
    g_z.start(lambda j: g_sum.at[pl.ds(multiple(j, 64), 64)])

    p_x.end(b["p_sum"])
    query_grad = b["p_sum"][...].T * scales + slopes * b["pos"][...].astype(F32)
    backward(b, 0, Q_ROWS, query_grad)
    weight_gradients(b, 0, Q_ROWS)

    g_z.wait()
    total = g_sum[pl.ds(multiple(z, 64), 64), :].astype(F32)
    for k in range(1, 8):
        total = total + b["g_z"][lax.rem(z + k, 8)].astype(F32)
    total = jnp.concatenate([total * inv_temp, jnp.zeros((64, 256), F32)], axis=0)
    backward(b, 1, N_ROWS, total)
    weight_gradients(b, 1, I_ROWS)

    outs = (o_first, o_second, o_third, o_loss)
    reduce_gradients(
        links, b["g_first"], b["g_second"], b["g_third"], loss_tile, outs, grad_bufs
    )
    links.finish()


def per_device(
    query_features,
    positive_features,
    negative_features,
    positive_ids,
    positive_counts,
    negative_ids,
    negative_counts,
    query_first,
    query_second,
    query_third,
    item_first,
    item_second,
    item_third,
):
    vmem = pl.BlockSpec(memory_space=pltpu.VMEM)
    anywhere = pl.BlockSpec(memory_space=pl.ANY)
    first, second, third, loss = pl.pallas_call(
        step_kernel,
        out_shape=(
            jax.ShapeDtypeStruct((2, 16, 1024), F32),
            jax.ShapeDtypeStruct((2, 32, 512), F32),
            jax.ShapeDtypeStruct((2, 16, 256), F32),
            jax.ShapeDtypeStruct((8, 128), F32),
        ),
        in_specs=[anywhere] * 9 + [vmem] * 4,
        out_specs=(vmem,) * 4,
        scratch_shapes=[
            STEP_BUFS,
            GRAD_BUFS,
            pltpu.SemaphoreType.DMA((9,)),
            pltpu.SemaphoreType.DMA((LINKS,)),
            pltpu.SemaphoreType.DMA((LINKS,)),
        ],
        compiler_params=pltpu.CompilerParams(
            collective_id=0, has_side_effects=True, vmem_limit_bytes=62 * 1024 * 1024
        ),
        name="training_step",
    )(
        query_features,
        positive_features,
        negative_features,
        query_first,
        query_second,
        query_third,
        item_first,
        item_second,
        item_third,
        positive_ids.astype(F32).reshape(1, 2048),
        positive_counts.reshape(2, 128),
        negative_ids.reshape(16, 128),
        negative_counts.reshape(16, 128),
    )
    queries = query_features.shape[0] * lax.axis_size(DP) * lax.axis_size(NEG)
    mean_loss = loss[0, 0] / queries
    return (mean_loss, first[0], second[0], third[0], first[1], second[1], third[1])


def solution(mesh):
    torus = Mesh(mesh.devices.reshape(4, 8, 4, 2), DP_NEG)
    placed = (
        P(DP_NEG, None),
        P(DP_NEG, None),
        P(NEG_DP, None),
        P(DP),
        P(DP_NEG),
        P(NEG),
        P(NEG),
        P(),
        P(),
        P(),
        P(),
        P(),
        P(),
    )
    return jax.shard_map(
        per_device,
        mesh=torus,
        in_specs=placed,
        out_specs=(P(),) + (P(DP, None),) * 6,
        check_vma=False,
    )
```

```python
import jax
import jax.numpy as jnp
from jax import lax
from jax.experimental import pallas as pl
from jax.experimental.pallas import tpu as pltpu
from jax.sharding import Mesh
from jax.sharding import PartitionSpec as P

NEG = ("neg_0", "neg_1")
DP = ("dp_0", "dp_1")
DP_NEG = ("dp_0", "dp_1", "neg_0", "neg_1")
NEG_DP = ("neg_0", "neg_1", "dp_0", "dp_1")
AX_Y, AX_Z, AX_X, AX_C = "dp_0", "dp_1", "neg_0", "neg_1"
MESH = pl.DeviceIdType.MESH
F32 = jnp.float32
BF16 = jnp.bfloat16

QUERIES = 65536
inv_temp = 20.0
clip_norm = 256.0
LOG2_E = 1.4426950408889634


class Links:
    def __init__(self, send_sems, recv_sems, size):
        self.send_sems, self.recv_sems, self.size = send_sems, recv_sems, size
        self.used = 0
        self.started = []

    def copy(self, src, dst, device):
        at = self.used
        self.used += 1
        assert at < self.size
        made = pltpu.make_async_remote_copy(
            src_ref=src,
            dst_ref=dst,
            send_sem=self.send_sems.at[at],
            recv_sem=self.recv_sems.at[at],
            device_id=device,
            device_id_type=MESH,
        )
        made.start()
        self.started.append(made)
        return made

    def finish(self):
        for made in self.started:
            made.wait_send()


def add_rows(out, terms, rows, step):
    def body(i, carry):
        at = pl.ds(pl.multiple_of(i * step, step), step)
        total = terms[0][at].astype(F32)
        for term in terms[1:]:
            total = total + term[at].astype(F32)
        out[at] = total.astype(out.dtype)
        return carry

    if rows == step:
        body(0, 0)
    else:
        lax.fori_loop(0, rows // step, body, 0)


class Phases:
    def __init__(self):
        self.scope = None

    def __call__(self, name):
        if self.scope is not None:
            self.scope.__exit__(None, None, None)
        self.scope = None
        if name is not None:
            self.scope = jax.named_scope(name)
            self.scope.__enter__()


class Ring4:
    def __init__(self, links, axis, cut, rows, land, step):
        self.links, self.axis, self.cut, self.rows, self.step = links, axis, cut, rows, step
        self.early_up, self.early_down, self.from_down, self.from_up = land
        me = lax.axis_index(axis)
        self.me = me
        self.up, self.down, self.far = lax.rem(me + 1, 4), lax.rem(me + 3, 4), lax.rem(me + 2, 4)
        half = rows // 2
        self.half, self.low, self.high = half, pl.ds(0, half), pl.ds(half, half)

    def start_far(self):
        far = self.cut(self.far)
        self.a = self.links.copy(far.at[self.low], self.early_up, {self.axis: self.up})
        self.b = self.links.copy(far.at[self.high], self.early_down, {self.axis: self.down})

    def start_near(self):
        self.c = self.links.copy(
            self.cut(self.up).at[self.high], self.from_down.at[self.high], {self.axis: self.up}
        )
        self.d = self.links.copy(
            self.cut(self.down).at[self.low], self.from_up.at[self.low], {self.axis: self.down}
        )

    def start(self):
        self.start_far()
        self.start_near()

    def relay(self):
        self.a.wait_recv()
        mine = self.cut(self.up).at[self.low]
        add_rows(self.early_up, (mine, self.early_up), self.half, self.step)
        self.e = self.links.copy(self.early_up, self.from_down.at[self.low], {self.axis: self.up})
        self.b.wait_recv()
        mine = self.cut(self.down).at[self.high]
        add_rows(self.early_down, (mine, self.early_down), self.half, self.step)
        self.f = self.links.copy(
            self.early_down, self.from_up.at[self.high], {self.axis: self.down}
        )

    def end(self, out):
        for made in (self.c, self.d, self.e, self.f):
            made.wait_recv()
        add_rows(out, (self.cut(self.me), self.from_down, self.from_up), self.rows, self.step)


class Direct:
    def __init__(self, links, axis, size, slots):
        self.links, self.axis, self.size, self.slots = links, axis, size, slots
        self.me = lax.axis_index(axis)

    def start(self, cut):
        self.made = []
        for k in range(1, self.size):
            to = lax.rem(self.me + k, self.size)
            self.made.append(self.links.copy(cut(to), self.slots.at[self.me], {self.axis: to}))

    def wait(self):
        for made in self.made:
            made.wait_recv()


def in_order(slots, count):
    total = slots[0].astype(F32)
    for j in range(1, count):
        total = total + slots[j].astype(F32)
    return total


def group_peers():
    x, c = lax.axis_index(AX_X), lax.axis_index(AX_C)
    peers = []
    for k in range(1, 8):
        other = lax.rem(x * 2 + c + k, 8)
        peers.append({AX_X: other // 2, AX_C: lax.rem(other, 2)})
    return peers


def plane_peers():
    y, z = lax.axis_index(AX_Y), lax.axis_index(AX_Z)
    peers = []
    for k in range(1, 32):
        other = lax.rem(y * 8 + z + k, 32)
        peers.append({AX_Y: other // 8, AX_Z: lax.rem(other, 8)})
    return peers


def greet_neighbours():
    barrier = pltpu.get_barrier_semaphore()
    peers = group_peers() + plane_peers()
    for peer in peers:
        pl.semaphore_signal(barrier, inc=1, device_id=peer, device_id_type=MESH)
    return barrier, len(peers)


def multiple(index, size):
    return pl.multiple_of(index * size, size)


class TowerSum:
    def __init__(self, links, b, g, t):
        self.links, self.b, self.t, self.g = links, b, t, g
        self.y, self.z, self.x, self.c = (lax.axis_index(a) for a in (AX_Y, AX_Z, AX_X, AX_C))

    def pair_first(self):
        columns = pl.ds(multiple(1 - self.c, 512), 512)
        mine = self.g["g_first"].at[self.t, :, :, columns]
        self.pair = [self.links.copy(mine, self.b["a_first"], {AX_C: 1 - self.c})]

    def pair_second(self):
        mine = self.g["g_second"].at[self.t, :, 1 - self.c]
        self.pair.append(self.links.copy(mine, self.b["a_second"], {AX_C: 1 - self.c}))

    def pair_third(self):
        columns = pl.ds(multiple(1 - self.c, 128), 128)
        mine = self.g["g_third"].at[self.t, :, :, :, columns]
        self.pair.append(self.links.copy(mine, self.b["a_third"], {AX_C: 1 - self.c}))

    def stage1(self):
        t, c, g, b, links = self.t, self.c, self.g, self.b, self.links
        first, second = b["a_first"], b["a_second"]
        self.pair[0].wait_recv()
        own = g["g_first"].at[t, :, :, pl.ds(multiple(c, 512), 512)]
        add_rows(first, (first, own), 32, 4)
        self.first_x = Ring4(
            links, AX_X, lambda j: first.at[:, :, pl.ds(multiple(j, 128), 128)], 32, b["fx"], 16
        )
        self.first_x.start()
        self.pair[1].wait_recv()
        add_rows(second, (second, g["g_second"].at[t, :, c]), 32, 4)
        self.second_y = Ring4(
            links, AX_Y, lambda j: second.at[pl.ds(multiple(j, 8), 8)], 8, b["sy"], 4
        )
        self.second_y.start()

    def third1(self):
        t, c, g, b, links = self.t, self.c, self.g, self.b, self.links
        third = b["a_third"]
        self.pair[2].wait_recv()
        own = g["g_third"].at[t, :, :, :, pl.ds(multiple(c, 128), 128)]
        add_rows(third, (third, own), 4, 1)
        self.third_z = Direct(links, AX_Z, 8, b["tz"])
        self.third_z.start(lambda j: third.at[:, j])

    def relay1(self):
        self.first_x.relay()
        self.second_y.relay()

    def third2(self):
        b = self.b
        self.third_z.wait()
        b["tz"][self.z] = b["a_third"][:, self.z]
        b["t_sum"][...] = in_order(b["tz"], 8).astype(BF16)
        self.third_y = Direct(self.links, AX_Y, 4, b["ty"])
        self.third_y.start(lambda j: b["t_sum"].at[j])

    def stage2(self):
        b, links = self.b, self.links
        fx_sum, sy_sum = b["fx_sum"], b["sy_sum"]
        self.first_x.end(fx_sum)
        self.first_y = Ring4(
            links, AX_Y, lambda j: fx_sum.at[pl.ds(multiple(j, 8), 8)], 8, b["fy"], 4
        )
        self.first_y.start()
        self.second_y.end(sy_sum)
        self.second_x = Ring4(
            links, AX_X, lambda j: sy_sum.at[:, :, pl.ds(multiple(j, 128), 128)], 8, b["sx"], 4
        )
        self.second_x.start()

    def third3(self):
        b = self.b
        self.third_y.wait()
        b["ty"][self.y] = b["t_sum"][self.y]
        b["ty_sum"][...] = in_order(b["ty"], 4).astype(BF16)
        self.third_x = Direct(self.links, AX_X, 4, b["tx"])
        self.third_x.start(lambda j: b["ty_sum"])

    def relay2(self):
        self.first_y.relay()
        self.second_x.relay()

    def stage3(self):
        b = self.b
        both = b["both"]
        self.first_y.end(both.at[:, 0])
        self.second_x.end(both.at[:, 1])
        self.last_z = Direct(self.links, AX_Z, 8, b["lz"])
        self.last_z.start(lambda j: both.at[j])

    def last(self):
        b, t = self.b, self.t
        self.third_x.wait()
        b["tx"][self.x] = b["ty_sum"][...]
        third = in_order(b["tx"], 4)
        self.last_z.wait()
        b["lz"][self.z] = b["both"][self.z]
        piece = in_order(b["lz"], 8)
        b["own"][...] = piece
        b["t_own"][...] = third
        squares = jnp.sum((piece * piece).reshape(4, 8, 128), axis=0)
        return squares + jnp.sum((third * third).reshape(2, 8, 128), axis=0) * 0.25

    def spread(self):
        b, me = self.b, self.x * 2 + self.c
        self.pieces = [self.links.copy(b["t_own"], b["ag_third"].at[self.c], {AX_C: 1 - self.c})]
        for peer in group_peers():
            self.pieces.append(self.links.copy(b["own"], b["ag"].at[me], peer))
        b["ag"][me] = b["own"][...]
        b["ag_third"][self.c] = b["t_own"][...]

    def collect(self, o_first, o_second, o_third):
        b = self.b
        for made in self.pieces:
            made.wait_recv()
        for cc in range(2):
            for xx in range(4):
                me = xx * 2 + cc
                o_first[:, pl.ds(cc * 512 + xx * 128, 128)] = b["ag"][me, 0]
                o_second[pl.ds(cc * 16, 16), pl.ds(xx * 128, 128)] = b["ag"][me, 1]
            o_third[:, pl.ds(cc * 128, 128)] = b["ag_third"][cc]


LINKS = 256


def ring_land(rows, *rest):
    half = pltpu.VMEM((rows // 2, *rest), BF16)
    whole = pltpu.VMEM((rows, *rest), BF16)
    return (half, half, whole, whole)


SUM_BUFS = {
    "a_first": pltpu.VMEM((32, 16, 512), BF16),
    "a_second": pltpu.VMEM((32, 16, 512), BF16),
    "a_third": pltpu.VMEM((4, 8, 16, 128), BF16),
    "fx": ring_land(32, 16, 128),
    "sy": ring_land(8, 16, 512),
    "tz": pltpu.VMEM((8, 4, 16, 128), BF16),
    "t_sum": pltpu.VMEM((4, 16, 128), BF16),
    "ty": pltpu.VMEM((4, 16, 128), BF16),
    "ty_sum": pltpu.VMEM((16, 128), BF16),
    "tx": pltpu.VMEM((4, 16, 128), BF16),
    "fx_sum": pltpu.VMEM((32, 16, 128), BF16),
    "sy_sum": pltpu.VMEM((8, 16, 512), BF16),
    "fy": ring_land(8, 16, 128),
    "sx": ring_land(8, 16, 128),
    "both": pltpu.VMEM((8, 2, 16, 128), BF16),
    "lz": pltpu.VMEM((8, 2, 16, 128), BF16),
    "own": pltpu.VMEM((2, 16, 128), F32),
    "t_own": pltpu.VMEM((16, 128), F32),
    "ag": pltpu.VMEM((8, 2, 16, 128), F32),
    "ag_third": pltpu.VMEM((2, 16, 128), F32),
}

SCALAR_BUFS = {
    "c_in": pltpu.VMEM((8, 8, 128), F32),
    "c_out": pltpu.VMEM((8, 128), F32),
    "p_in": pltpu.VMEM((32, 8, 128), F32),
    "p_out": pltpu.VMEM((8, 128), F32),
    "total": pltpu.VMEM((8, 128), F32),
}


ROWS = pl.ds(0, 4)


class Scalars:
    def __init__(self, links, b):
        self.links, self.b = links, b

    def start(self, squares):
        b, links = self.b, self.links
        me = lax.axis_index(AX_X) * 2 + lax.axis_index(AX_C)
        b["c_out"][0:1] = jnp.sum(squares, axis=0, keepdims=True)
        self.made = [links.copy(b["c_out"].at[ROWS], b["c_in"].at[me, ROWS], peer) for peer in group_peers()]
        b["c_in"][me, ROWS] = b["c_out"][ROWS]

    def over_plane(self):
        b, links = self.b, self.links
        d = lax.axis_index(AX_Y) * 8 + lax.axis_index(AX_Z)
        for made in self.made:
            made.wait_recv()
        b["p_out"][ROWS] = in_order(b["c_in"].at[:, ROWS], 8)
        self.made = [links.copy(b["p_out"].at[ROWS], b["p_in"].at[d, ROWS], peer) for peer in plane_peers()]
        b["p_in"][d, ROWS] = b["p_out"][ROWS]

    def end(self):
        for made in self.made:
            made.wait_recv()
        self.b["total"][ROWS] = in_order(self.b["p_in"].at[:, ROWS], 32)
        return self.b["total"][...]


Q_ROWS, P_ROWS, N_ROWS = pl.ds(0, 256), pl.ds(256, 256), pl.ds(512, 128)
I_ROWS = pl.ds(256, 384)

STEP_BUFS = {
    "pos_ids": pltpu.VMEM((16, 128), jnp.int32),
    "pos_counts": pltpu.VMEM((2, 128), jnp.int32),
    "neg_ids": pltpu.VMEM((16, 128), jnp.int32),
    "neg_counts": pltpu.VMEM((16, 128), jnp.int32),
    "w1": pltpu.VMEM((2, 512, 1024), BF16),
    "w2": pltpu.VMEM((2, 1024, 512), BF16),
    "w3": pltpu.VMEM((2, 512, 256), BF16),
    "x": pltpu.VMEM((640, 512), BF16),
    "a1": pltpu.VMEM((640, 1024), BF16),
    "a2": pltpu.VMEM((640, 512), BF16),
    "s1": pltpu.VMEM((640, 1024), F32),
    "s2": pltpu.VMEM((640, 512), F32),
    "emb": pltpu.VMEM((640, 256), F32),
    "inv": pltpu.VMEM((640, 1), F32),
    "eg": pltpu.VMEM((640, 256), BF16),
    "d2": pltpu.VMEM((640, 512), BF16),
    "d1": pltpu.VMEM((640, 1024), BF16),
    "xt": pltpu.VMEM((512, 640), BF16),
    "a1t": pltpu.VMEM((1024, 640), BF16),
    "a2t": pltpu.VMEM((512, 640), BF16),
    "eye": pltpu.VMEM((256, 256), BF16),
    "pos": pltpu.VMEM((256, 256), BF16),
    "q": pltpu.VMEM((2048, 256), BF16),
    "qs": pltpu.VMEM((2048, 256), BF16),
    "n": pltpu.VMEM((2048, 256), BF16),
    "nt": pltpu.VMEM((256, 2048), BF16),
    "et": pltpu.VMEM((2048, 2048), BF16),
    "turn": pltpu.VMEM((128, 128), F32),
    "ids": pltpu.VMEM((2048, 128), F32),
    "log": pltpu.VMEM((2048, 128), F32),
    "part": pltpu.VMEM((8, 2048), F32),
    "den_out": pltpu.VMEM((16, 128), F32),
    "den_in": pltpu.VMEM((8, 16, 128), F32),
    "den": pltpu.VMEM((16, 128), F32),
    "p_out": pltpu.VMEM((2, 4, 256, 256), BF16),
    "p_pair": pltpu.VMEM((4, 256, 256), BF16),
    "p_ring": ring_land(256, 256),
    "p_sum": pltpu.VMEM((256, 256), F32),
    "g_out": pltpu.VMEM((2048, 256), BF16),
    "g_ring": ring_land(512, 256),
    "g_sum": pltpu.VMEM((512, 256), BF16),
    "g_z": pltpu.VMEM((8, 64, 256), BF16),
    "g_first": pltpu.VMEM((2, 32, 16, 1024), BF16),
    "g_second": pltpu.VMEM((2, 32, 2, 16, 512), BF16),
    "g_third": pltpu.VMEM((2, 4, 8, 16, 256), BF16),
    "sum_query": SUM_BUFS,
    "sum_item": SUM_BUFS,
    "scalars": SCALAR_BUFS,
}


def dot(a, b):
    return jnp.dot(a, b, preferred_element_type=F32)


def dot_cols(a, b):
    return lax.dot_general(a, b, (((1,), (1,)), ((), ())), preferred_element_type=F32)


def silu_both(pre):
    sigma = 0.5 * jnp.tanh(0.5 * pre) + 0.5
    act = pre * sigma
    return act, sigma * (1.0 + pre - act)


def forward(b, t, rows, loads=()):
    def layer(i, carry):
        cols = pl.ds(multiple(i, 512), 512)
        act, slope = silu_both(dot(b["x"][rows, :], b["w1"][t, :, cols]))
        b["a1"][rows, cols] = act.astype(BF16)
        b["s1"][rows, cols] = slope
        return carry

    lax.fori_loop(0, 2, layer, 0)
    for made in loads:
        made.wait()
    act, slope = silu_both(dot(b["a1"][rows, :], b["w2"][t]))
    b["a2"][rows, :] = act.astype(BF16)
    b["s2"][rows, :] = slope
    embedding = dot(b["a2"][rows, :], b["w3"][t])
    inv_norm = lax.rsqrt(jnp.sum(embedding * embedding, axis=1, keepdims=True) + 1.0)
    b["emb"][rows, :] = embedding
    b["inv"][rows, :] = inv_norm
    return (embedding * inv_norm).astype(BF16)


def backward(b, t, rows, unit_grad):
    embedding, inv_norm = b["emb"][rows, :], b["inv"][rows, :]
    along = jnp.sum(embedding * unit_grad, axis=1, keepdims=True)
    embed_grad = inv_norm * unit_grad - inv_norm * inv_norm * inv_norm * embedding * along
    b["eg"][rows, :] = embed_grad.astype(BF16)
    slope = dot_cols(b["eg"][rows, :], b["w3"][t]) * b["s2"][rows, :]
    b["d2"][rows, :] = slope.astype(BF16)

    def layer(i, carry):
        cols = pl.ds(multiple(i, 512), 512)
        slope = dot_cols(b["d2"][rows, :], b["w2"][t, cols, :]) * b["s1"][rows, cols]
        b["d1"][rows, cols] = slope.astype(BF16)
        return carry

    lax.fori_loop(0, 2, layer, 0)


def weight_gradients(b, t, rows, tower):
    def first(i, carry):
        cols = pl.ds(multiple(i, 512), 512)
        made = dot(b["xt"][:, rows], b["d1"][rows, cols]).astype(BF16)
        b["g_first"][t, :, :, cols] = made.reshape(32, 16, 512)
        return carry

    lax.fori_loop(0, 2, first, 0)
    tower.pair_first()

    def second(i, carry):
        at = pl.ds(multiple(i, 512), 512)
        made = dot(b["a1t"][at, rows], b["d2"][rows, :]).astype(BF16)
        b["g_second"][t, pl.ds(multiple(i, 16), 16)] = made.reshape(16, 2, 16, 512)
        return carry

    lax.fori_loop(0, 2, second, 0)
    tower.pair_second()
    third = dot(b["a2t"][:, rows], b["eg"][rows, :]).astype(BF16)
    b["g_third"][t] = third.reshape(4, 8, 16, 256)
    tower.pair_third()


def turn_activations(b, rows):
    for name, cols in (("x", 512), ("a1", 1024), ("a2", 512)):

        def block(i, carry, name=name):
            at = pl.ds(multiple(i, 256), 256)
            turned = dot_cols(b["eye"][...], b[name][rows, at])
            b[name + "t"][at, rows] = turned.astype(BF16)
            return carry

        lax.fori_loop(0, cols // 256, block, 0)


def column(row):
    return jnp.broadcast_to(row, (128, 128)).T


def turn_negatives(b, u):
    for h in range(2):
        half = pl.ds(pl.multiple_of(u * 512 + h * 256, 256), 256)
        b["nt"][:, half] = dot_cols(b["eye"][...], b["n"][half, :]).astype(BF16)


def score_tile(b, pos_ids, u, i):
    at, cols = pl.ds(multiple(u, 512), 512), pl.ds(multiple(i, 512), 512)
    products = dot_cols(b["n"][at, :], b["q"][cols, :])
    logs = jnp.concatenate([b["log"][at, :]] * 4, axis=1)
    ids = jnp.concatenate([b["ids"][at, :]] * 4, axis=1)
    weights = jnp.exp2(products * (inv_temp * LOG2_E) - logs)
    rows = [pos_ids[pl.ds(i * 4 + r, 1), :].astype(F32) for r in range(4)]
    weights = jnp.where(jnp.concatenate(rows, axis=1) != ids, weights, 0.0)
    b["et"][at, cols] = weights.astype(BF16)
    b["part"][:, cols] += jnp.sum(weights.reshape(64, 8, 512), axis=0)


def step_kernel(
    query_x,
    positive_x,
    negative_x,
    q1,
    q2,
    q3,
    i1,
    i2,
    i3,
    pos_ids_in,
    pos_counts_in,
    neg_ids_in,
    neg_counts_in,
    o_query_first,
    o_query_second,
    o_query_third,
    o_item_first,
    o_item_second,
    o_item_third,
    o_scalars,
    b,
    load,
    send,
    recv,
):
    y, z, x, c = (lax.axis_index(a) for a in (AX_Y, AX_Z, AX_X, AX_C))
    me = x * 2 + c
    barrier, peers = greet_neighbours()
    links = Links(send, recv, LINKS)
    phase = Phases()
    phase("load")

    loads = [
        (negative_x, b["x"].at[pl.ds(512, 64)]),
        (i1, b["w1"].at[1]),
        (i2, b["w2"].at[1]),
        (i3, b["w3"].at[1]),
        (query_x, b["x"].at[Q_ROWS]),
        (q1, b["w1"].at[0]),
        (q2, b["w2"].at[0]),
        (q3, b["w3"].at[0]),
        (positive_x, b["x"].at[P_ROWS]),
        (pos_ids_in, b["pos_ids"]),
        (pos_counts_in, b["pos_counts"]),
        (neg_ids_in, b["neg_ids"]),
        (neg_counts_in, b["neg_counts"]),
    ]
    loads = [pltpu.make_async_copy(s, d, load.at[k]) for k, (s, d) in enumerate(loads)]
    for made in loads:
        made.start()

    b["x"][pl.ds(576, 64), :] = jnp.zeros((64, 512), BF16)
    b["part"][...] = jnp.zeros((8, 2048), F32)
    b["scalars"]["c_out"][...] = jnp.zeros((8, 128), F32)
    b["scalars"]["total"][...] = jnp.zeros((8, 128), F32)
    ones = lax.broadcasted_iota(jnp.int32, (256, 256), 0) == lax.broadcasted_iota(
        jnp.int32, (256, 256), 1
    )
    b["eye"][...] = jnp.where(ones, 1.0, 0.0).astype(BF16)

    loads[0].wait()
    loads[1].wait()
    phase("f_neg")
    n = b["n"]
    unit = forward(b, 1, N_ROWS, loads[2:4])

    def n_block(yy, zz):
        return n.at[pl.ds(pl.multiple_of((yy * 8 + zz) * 64, 64), 64)]

    def n_half(yy, zz, h):
        return n.at[pl.ds(pl.multiple_of((yy * 8 + zz) * 64 + h * 32, 32), 32)]

    n[pl.ds(pl.multiple_of((y * 8 + z) * 64, 64), 64), :] = unit[:64]
    phase("barrier")
    pl.semaphore_wait(barrier, peers)
    y_up, y_down = lax.rem(y + 1, 4), lax.rem(y + 3, 4)
    order = (1, 7, 2, 6, 3, 5, 4)
    n_z, n_y = {}, {}
    for k in order:
        n_z[k] = links.copy(n_block(y, z), n_block(y, z), {AX_Z: lax.rem(z + k, 8)})

    def n_forward(k):
        zz = lax.rem(z - k + 8, 8)
        n_y[k] = (
            links.copy(n_block(y, zz), n_block(y, zz), {AX_Y: y_up}),
            links.copy(n_block(y, zz), n_block(y, zz), {AX_Y: y_down}),
        )

    n_forward(0)

    phase("f_query")
    for made in loads[4:8]:
        made.wait()
    q = b["q"]
    q_own = forward(b, 0, Q_ROWS)

    def q_block(xx, cc):
        return q.at[pl.ds(pl.multiple_of((xx * 2 + cc) * 256, 256), 256)]

    def q_half(xx, cc, h):
        return q.at[pl.ds(pl.multiple_of((xx * 2 + cc) * 256 + h * 128, 128), 128)]

    q[pl.ds(multiple(me, 256), 256), :] = q_own
    x_up, x_down, x_far = lax.rem(x + 1, 4), lax.rem(x + 3, 4), lax.rem(x + 2, 4)
    other = {AX_C: 1 - c}
    q_up = links.copy(q_block(x, c), q_block(x, c), {AX_X: x_up})
    q_down = links.copy(q_block(x, c), q_block(x, c), {AX_X: x_down})
    q_pair = [links.copy(q_block(x, c), q_block(x, c), other)]

    phase("f_pos")
    for made in loads[8:]:
        made.wait()
    pos_ids, pos_counts, neg_ids, neg_counts = (
        b[k] for k in ("pos_ids", "pos_counts", "neg_ids", "neg_counts")
    )
    b["pos"][...] = forward(b, 1, P_ROWS)

    phase("n_fwd1")
    for k in order[:4]:
        n_z[k].wait_recv()
        n_forward(k)
    phase("q_relay")
    q_up.wait_recv()
    q_low = links.copy(q_half(x_down, c, 0), q_half(x_down, c, 0), {AX_X: x_up})
    q_pair.append(links.copy(q_block(x_down, c), q_block(x_down, c), other))
    q_down.wait_recv()
    q_high = links.copy(q_half(x_up, c, 1), q_half(x_up, c, 1), {AX_X: x_down})
    q_pair.append(links.copy(q_block(x_up, c), q_block(x_up, c), other))

    phase("small")
    turn = b["turn"]
    turn[...] = jnp.zeros((128, 128), F32)
    turn[pl.ds(0, 16), :] = neg_ids[...].astype(F32)
    turn[pl.ds(16, 16), :] = jnp.log(neg_counts[...].astype(F32)) * LOG2_E
    turned = turn[...].T
    for j in range(16):
        b["ids"][pl.ds(j * 128, 128), :] = jnp.broadcast_to(turned[:, j : j + 1], (128, 128))
        b["log"][pl.ds(j * 128, 128), :] = jnp.broadcast_to(
            turned[:, 16 + j : 17 + j], (128, 128)
        )
    phase("n_fwd2")
    for k in order[4:]:
        n_z[k].wait_recv()
        n_forward(k)

    n_far = []

    def n_relay(*which):
        for k in which:
            zz = lax.rem(z - k + 8, 8)
            from_down, from_up = n_y[k]
            from_down.wait_recv()
            n_far.append(
                links.copy(n_half(y_down, zz, 0), n_half(y_down, zz, 0), {AX_Y: y_up})
            )
            from_up.wait_recv()
            n_far.append(
                links.copy(n_half(y_up, zz, 1), n_half(y_up, zz, 1), {AX_Y: y_down})
            )

    phase("relay_a")
    n_relay(0, 1, 7)
    q_pair[0].wait_recv()
    phase("tile_a")
    score_tile(b, pos_ids, y, x)
    phase("relay_b")
    n_relay(2, 6)
    q_pair[1].wait_recv()
    phase("tile_b")
    score_tile(b, pos_ids, y, x_down)
    phase("relay_c")
    q_low.wait_recv()
    q_pair.append(links.copy(q_half(x_far, c, 0), q_half(x_far, c, 0), other))
    q_high.wait_recv()
    q_pair.append(links.copy(q_half(x_far, c, 1), q_half(x_far, c, 1), other))
    n_relay(3, 5)
    q_pair[2].wait_recv()
    phase("tile_c")
    score_tile(b, pos_ids, y, x_up)
    phase("relay_d")
    n_relay(4)
    phase("tiles")
    for made in q_pair[3:]:
        made.wait_recv()
    score_tile(b, pos_ids, y, x_far)

    def near_tiles(i, carry):
        score_tile(b, pos_ids, y_up, i)
        score_tile(b, pos_ids, y_down, i)
        return carry

    lax.fori_loop(0, 4, near_tiles, 0)
    phase("logits")
    own = b["q"][pl.ds(multiple(me, 256), 256), :].astype(F32)
    along = jnp.sum(own * b["pos"][...].astype(F32), axis=1, keepdims=True)
    logits = []
    for h in range(2):
        row = jnp.broadcast_to(along[h * 128 : (h + 1) * 128], (128, 128)).T[0:1, :]
        logits.append(row * inv_temp - jnp.log(pos_counts[h : h + 1, :].astype(F32)))

    phase("n_far")
    for made in n_far:
        made.wait_recv()
    phase("far_tiles")
    y_far = lax.rem(y + 2, 4)

    def far_tiles(i, carry):
        score_tile(b, pos_ids, y_far, i)
        return carry

    lax.fori_loop(0, 4, far_tiles, 0)

    phase("den")
    den_out, den_in = b["den_out"], b["den_in"]
    for j in range(16):
        den_out[pl.ds(j, 1), :] = jnp.sum(b["part"][:, j * 128 : (j + 1) * 128], axis=0, keepdims=True)
    for h in range(2):
        at = pl.ds(me * 2 + h, 1)
        den_out[at, :] = den_out[at, :] + jnp.exp(logits[h])
    sums = [links.copy(den_out, den_in.at[me], peer) for peer in group_peers()]
    den_in[me] = den_out[...]

    def turned(u, carry):
        turn_negatives(b, u)
        return carry

    lax.fori_loop(0, 4, turned, 0)

    phase("p_theirs")
    p_out = b["p_out"]

    def query_block(cc, i):
        cols = pl.ds(pl.multiple_of((i * 2 + cc) * 256, 256), 256)
        p_out[cc, i] = dot(b["nt"][...], b["et"][:, cols]).astype(BF16)

    def theirs(i, carry):
        query_block(1 - c, i)
        return carry

    def ours(i, carry):
        query_block(c, i)
        return carry

    lax.fori_loop(0, 4, theirs, 0)
    p_pair = b["p_pair"]
    pair = links.copy(p_out.at[1 - c], p_pair, other)
    phase("p_ours")
    lax.fori_loop(0, 4, ours, 0)
    phase("p_add")
    pair.wait_recv()
    for i in range(4):
        add_rows(p_pair.at[i], (p_pair.at[i], p_out.at[c, i]), 256, 64)
    p_x = Ring4(links, AX_X, lambda j: p_pair.at[j], 256, b["p_ring"], 128)
    p_x.start()

    phase("den_wait")
    for made in sums:
        made.wait_recv()
    total = in_order(den_in, 8)
    b["den"][...] = total
    turn[pl.ds(0, 16), :] = 1.0 / total
    turned = turn[...].T
    for j in range(16):
        at = pl.ds(j * 128, 128)
        b["qs"][at, :] = (q[at, :].astype(F32) * turned[:, j : j + 1]).astype(BF16)

    phase("g_rows")
    g_out = b["g_out"]

    def negative_rows(u):
        at = pl.ds(multiple(u, 512), 512)
        g_out[at, :] = dot(b["et"][at, :], b["qs"][...]).astype(BF16)

    g_y = Ring4(links, AX_Y, lambda j: g_out.at[pl.ds(multiple(j, 512), 512)], 512, b["g_ring"], 64)
    negative_rows(g_y.far)
    g_y.start_far()
    negative_rows(g_y.up)
    negative_rows(g_y.down)
    g_y.start_near()
    phase("p_relay")
    p_x.relay()
    phase("g_own")
    negative_rows(g_y.me)

    phase("slopes")
    losses, slopes, scales = [], [], []
    for h in range(2):
        den = b["den"][pl.ds(me * 2 + h, 1), :]
        losses.append(jnp.log(den) - logits[h])
        slope = column(jnp.exp(logits[h]) / den - 1.0) * inv_temp
        slopes.append(jnp.concatenate([slope, slope], axis=1))
        scale = column(inv_temp / den)
        scales.append(jnp.concatenate([scale, scale], axis=1))
    slopes = jnp.concatenate(slopes, axis=0)
    scales = jnp.concatenate(scales, axis=0)
    for h in range(2):
        b["scalars"]["c_out"][h + 1 : h + 2] = losses[h]
    phase("b_pos")
    own = q[pl.ds(multiple(me, 256), 256), :].astype(F32)
    backward(b, 1, P_ROWS, slopes * own)
    phase("g_relay")
    g_y.relay()
    phase("turn_q")
    turn_activations(b, Q_ROWS)

    phase("p_end")
    p_x.end(b["p_sum"])
    query_grad = b["p_sum"][...].T * scales + slopes * b["pos"][...].astype(F32)
    phase("b_query")
    backward(b, 0, Q_ROWS, query_grad)
    phase("w_query")
    query_sum = TowerSum(links, b["sum_query"], b, 0)
    item_sum = TowerSum(links, b["sum_item"], b, 1)
    weight_gradients(b, 0, Q_ROWS, query_sum)
    phase("g_end")
    g_sum = b["g_sum"]
    g_y.end(g_sum)
    g_z = Direct(links, AX_Z, 8, b["g_z"])
    g_z.start(lambda j: g_sum.at[pl.ds(multiple(j, 64), 64)])

    phase("q_stage1")
    query_sum.stage1()
    phase("turn_p")
    turn_activations(b, P_ROWS)
    phase("q_relay1")
    query_sum.relay1()
    phase("turn_n")
    turn_activations(b, N_ROWS)

    phase("g_z")
    g_z.wait()
    total = g_sum[pl.ds(multiple(z, 64), 64), :].astype(F32)
    for k in range(1, 8):
        total = total + b["g_z"][lax.rem(z + k, 8)].astype(F32)
    total = jnp.concatenate([total * inv_temp, jnp.zeros((64, 256), F32)], axis=0)
    phase("b_neg")
    backward(b, 1, N_ROWS, total)
    phase("q_stage2")
    query_sum.stage2()
    query_sum.third1()
    phase("w_item")
    weight_gradients(b, 1, I_ROWS, item_sum)
    phase("q_relay2")
    query_sum.relay2()
    phase("i_stage1")
    item_sum.stage1()
    item_sum.third1()
    phase("q_third2")
    query_sum.third2()
    phase("q_stage3")
    query_sum.stage3()
    phase("i_relay1")
    item_sum.relay1()
    phase("i_stage2")
    item_sum.stage2()
    phase("q_third3")
    query_sum.third3()
    item_sum.third2()
    phase("i_relay2")
    item_sum.relay2()
    item_sum.third3()
    phase("q_last")
    squares = query_sum.last()
    query_sum.spread()
    phase("i_stage3")
    item_sum.stage3()
    phase("i_last")
    squares = squares + item_sum.last()
    scalars = Scalars(links, b["scalars"])
    scalars.start(squares)
    item_sum.spread()
    phase("group")
    scalars.over_plane()
    phase("plane")
    total = scalars.end()
    row = lax.broadcasted_iota(jnp.int32, (8, 128), 0)
    norm = jnp.sqrt(jnp.sum(jnp.where(row == 0, total, 0.0), keepdims=True))
    factor = clip_norm / jnp.maximum(norm, clip_norm)
    o_scalars[0] = jnp.broadcast_to(factor, (8, 128))
    o_scalars[1] = jnp.broadcast_to(jnp.sum(jnp.where((row == 1) | (row == 2), total, 0.0), keepdims=True), (8, 128))
    phase("pieces")
    query_sum.collect(o_query_first, o_query_second, o_query_third)
    item_sum.collect(o_item_first, o_item_second, o_item_third)
    phase("finish")
    links.finish()
    phase(None)


def clip_kernel(*refs):
    scalars, raw, clipped, loss = refs[0], refs[1:7], refs[7:13], refs[13]
    factor = scalars[0, 0:1, 0:1]
    for source, result in zip(raw, clipped):
        result[...] = source[...] * factor
    loss[...] = scalars[1, 0:1, 0:1] * (1.0 / QUERIES)


def per_device(
    query_features,
    positive_features,
    negative_features,
    positive_ids,
    positive_counts,
    negative_ids,
    negative_counts,
    query_first,
    query_second,
    query_third,
    item_first,
    item_second,
    item_third,
):
    vmem = pl.BlockSpec(memory_space=pltpu.VMEM)
    anywhere = pl.BlockSpec(memory_space=pl.ANY)
    tower = (
        jax.ShapeDtypeStruct((16, 1024), F32),
        jax.ShapeDtypeStruct((32, 512), F32),
        jax.ShapeDtypeStruct((16, 256), F32),
    )
    *raw, scalars = pl.pallas_call(
        step_kernel,
        out_shape=tower + tower + (jax.ShapeDtypeStruct((2, 8, 128), F32),),
        in_specs=[anywhere] * 13,
        out_specs=(vmem,) * 7,
        scratch_shapes=[
            STEP_BUFS,
            pltpu.SemaphoreType.DMA((13,)),
            pltpu.SemaphoreType.DMA((LINKS,)),
            pltpu.SemaphoreType.DMA((LINKS,)),
        ],
        compiler_params=pltpu.CompilerParams(
            collective_id=0, has_side_effects=True, vmem_limit_bytes=56 * 1024 * 1024
        ),
        name="training_step",
    )(
        query_features,
        positive_features,
        negative_features,
        query_first,
        query_second,
        query_third,
        item_first,
        item_second,
        item_third,
        positive_ids.reshape(16, 128),
        positive_counts.reshape(2, 128),
        negative_ids.reshape(16, 128),
        negative_counts.reshape(16, 128),
    )
    *clipped, loss = pl.pallas_call(
        clip_kernel,
        out_shape=tower + tower + (jax.ShapeDtypeStruct((1, 1), F32),),
        in_specs=[vmem] * 7,
        out_specs=(vmem,) * 7,
        name="clip",
    )(scalars, *raw)
    return (loss.reshape(()), *clipped)


def solution(mesh):
    torus = Mesh(mesh.devices.reshape(4, 8, 4, 2), DP_NEG)
    placed = (
        P(DP_NEG, None),
        P(DP_NEG, None),
        P(NEG_DP, None),
        P(DP),
        P(DP_NEG),
        P(NEG),
        P(NEG),
        P(),
        P(),
        P(),
        P(),
        P(),
        P(),
    )
    return jax.shard_map(
        per_device,
        mesh=torus,
        in_specs=placed,
        out_specs=(P(),) + (P(DP, None),) * 6,
        check_vma=False,
    )
```

```python
import jax
import jax.numpy as jnp
from jax import lax
from jax.experimental import pallas as pl
from jax.experimental.pallas import tpu as pltpu
from jax.sharding import Mesh
from jax.sharding import PartitionSpec as P

NEG = ("neg_0", "neg_1")
DP = ("dp_0", "dp_1")
DP_NEG = ("dp_0", "dp_1", "neg_0", "neg_1")
NEG_DP = ("neg_0", "neg_1", "dp_0", "dp_1")
AX_Y, AX_Z, AX_X, AX_C = "dp_0", "dp_1", "neg_0", "neg_1"
MESH = pl.DeviceIdType.MESH
F32 = jnp.float32
BF16 = jnp.bfloat16

QUERIES = 65536
inv_temp = 20.0
clip_norm = 256.0
LOG2_E = 1.4426950408889634


class Links:
    def __init__(self, send_sems, recv_sems, size):
        self.send_sems, self.recv_sems, self.size = send_sems, recv_sems, size
        self.used = 0
        self.started = []

    def copy(self, src, dst, device):
        at = self.used
        self.used += 1
        assert at < self.size
        made = pltpu.make_async_remote_copy(
            src_ref=src,
            dst_ref=dst,
            send_sem=self.send_sems.at[at],
            recv_sem=self.recv_sems.at[at],
            device_id=device,
            device_id_type=MESH,
        )
        made.start()
        self.started.append(made)
        return made

    def finish(self):
        for made in self.started:
            made.wait_send()


def add_rows(out, terms, rows, step):
    def body(i, carry):
        at = pl.ds(pl.multiple_of(i * step, step), step)
        total = terms[0][at].astype(F32)
        for term in terms[1:]:
            total = total + term[at].astype(F32)
        out[at] = total.astype(out.dtype)
        return carry

    if rows == step:
        body(0, 0)
    else:
        lax.fori_loop(0, rows // step, body, 0)


class Phases:
    def __init__(self):
        self.scope = None

    def __call__(self, name):
        if self.scope is not None:
            self.scope.__exit__(None, None, None)
        self.scope = None
        if name is not None:
            self.scope = jax.named_scope(name)
            self.scope.__enter__()


class Ring4:
    def __init__(self, links, axis, cut, rows, land, step):
        self.links, self.axis, self.cut, self.rows, self.step = links, axis, cut, rows, step
        self.early_up, self.early_down, self.from_down, self.from_up = land
        me = lax.axis_index(axis)
        self.me = me
        self.up, self.down, self.far = lax.rem(me + 1, 4), lax.rem(me + 3, 4), lax.rem(me + 2, 4)
        half = rows // 2
        self.half, self.low, self.high = half, pl.ds(0, half), pl.ds(half, half)

    def start_far(self):
        far = self.cut(self.far)
        self.a = self.links.copy(far.at[self.low], self.early_up, {self.axis: self.up})
        self.b = self.links.copy(far.at[self.high], self.early_down, {self.axis: self.down})

    def start_near(self):
        self.c = self.links.copy(
            self.cut(self.up).at[self.high], self.from_down.at[self.high], {self.axis: self.up}
        )
        self.d = self.links.copy(
            self.cut(self.down).at[self.low], self.from_up.at[self.low], {self.axis: self.down}
        )

    def start(self):
        self.start_far()
        self.start_near()

    def relay(self):
        self.a.wait_recv()
        mine = self.cut(self.up).at[self.low]
        add_rows(self.early_up, (mine, self.early_up), self.half, self.step)
        self.e = self.links.copy(self.early_up, self.from_down.at[self.low], {self.axis: self.up})
        self.b.wait_recv()
        mine = self.cut(self.down).at[self.high]
        add_rows(self.early_down, (mine, self.early_down), self.half, self.step)
        self.f = self.links.copy(
            self.early_down, self.from_up.at[self.high], {self.axis: self.down}
        )

    def end(self, out):
        for made in (self.c, self.d, self.e, self.f):
            made.wait_recv()
        add_rows(out, (self.cut(self.me), self.from_down, self.from_up), self.rows, self.step)


class Direct:
    def __init__(self, links, axis, size, slots):
        self.links, self.axis, self.size, self.slots = links, axis, size, slots
        self.me = lax.axis_index(axis)

    def start(self, cut):
        self.made = []
        for k in range(1, self.size):
            to = lax.rem(self.me + k, self.size)
            self.made.append(self.links.copy(cut(to), self.slots.at[self.me], {self.axis: to}))

    def wait(self):
        for made in self.made:
            made.wait_recv()


def in_order(slots, count):
    total = slots[0].astype(F32)
    for j in range(1, count):
        total = total + slots[j].astype(F32)
    return total


def group_peers():
    x, c = lax.axis_index(AX_X), lax.axis_index(AX_C)
    peers = []
    for k in range(1, 8):
        other = lax.rem(x * 2 + c + k, 8)
        peers.append({AX_X: other // 2, AX_C: lax.rem(other, 2)})
    return peers


def plane_peers():
    y, z = lax.axis_index(AX_Y), lax.axis_index(AX_Z)
    peers = []
    for k in range(1, 32):
        other = lax.rem(y * 8 + z + k, 32)
        peers.append({AX_Y: other // 8, AX_Z: lax.rem(other, 8)})
    return peers


def greet_neighbours():
    barrier = pltpu.get_barrier_semaphore()
    peers = group_peers() + plane_peers()
    for peer in peers:
        pl.semaphore_signal(barrier, inc=1, device_id=peer, device_id_type=MESH)
    return barrier, len(peers)


def multiple(index, size):
    return pl.multiple_of(index * size, size)


class TowerSum:
    def __init__(self, links, b, g, t):
        self.links, self.b, self.t, self.g = links, b, t, g
        self.y, self.z, self.x, self.c = (lax.axis_index(a) for a in (AX_Y, AX_Z, AX_X, AX_C))

    def pair_first(self):
        columns = pl.ds(multiple(1 - self.c, 512), 512)
        mine = self.g["g_first"].at[self.t, :, :, columns]
        self.pair = [self.links.copy(mine, self.b["a_first"], {AX_C: 1 - self.c})]

    def pair_second(self):
        mine = self.g["g_second"].at[self.t, :, 1 - self.c]
        self.pair.append(self.links.copy(mine, self.b["a_second"], {AX_C: 1 - self.c}))

    def pair_third(self):
        columns = pl.ds(multiple(1 - self.c, 128), 128)
        mine = self.g["g_third"].at[self.t, :, :, :, columns]
        self.pair.append(self.links.copy(mine, self.b["a_third"], {AX_C: 1 - self.c}))

    def stage1(self):
        t, c, g, b, links = self.t, self.c, self.g, self.b, self.links
        first, second = b["a_first"], b["a_second"]
        self.pair[0].wait_recv()
        own = g["g_first"].at[t, :, :, pl.ds(multiple(c, 512), 512)]
        add_rows(first, (first, own), 32, 4)
        self.first_x = Ring4(
            links, AX_X, lambda j: first.at[:, :, pl.ds(multiple(j, 128), 128)], 32, b["fx"], 16
        )
        self.first_x.start()
        self.pair[1].wait_recv()
        add_rows(second, (second, g["g_second"].at[t, :, c]), 32, 4)
        self.second_y = Ring4(
            links, AX_Y, lambda j: second.at[pl.ds(multiple(j, 8), 8)], 8, b["sy"], 4
        )
        self.second_y.start()

    def third1(self):
        t, c, g, b, links = self.t, self.c, self.g, self.b, self.links
        third = b["a_third"]
        self.pair[2].wait_recv()
        own = g["g_third"].at[t, :, :, :, pl.ds(multiple(c, 128), 128)]
        add_rows(third, (third, own), 4, 1)
        self.third_z = Direct(links, AX_Z, 8, b["tz"])
        self.third_z.start(lambda j: third.at[:, j])

    def relay1(self):
        self.first_x.relay()
        self.second_y.relay()

    def third2(self):
        b = self.b
        self.third_z.wait()
        b["tz"][self.z] = b["a_third"][:, self.z]
        b["t_sum"][...] = in_order(b["tz"], 8).astype(BF16)
        self.third_y = Direct(self.links, AX_Y, 4, b["ty"])
        self.third_y.start(lambda j: b["t_sum"].at[j])

    def stage2(self):
        b, links = self.b, self.links
        fx_sum, sy_sum = b["fx_sum"], b["sy_sum"]
        self.first_x.end(fx_sum)
        self.first_y = Direct(links, AX_Y, 4, b["fy"])
        self.first_y.start(lambda j: fx_sum.at[pl.ds(multiple(j, 8), 8)])
        self.second_y.end(sy_sum)
        self.second_x = Direct(links, AX_X, 4, b["sx"])
        self.second_x.start(lambda j: sy_sum.at[:, :, pl.ds(multiple(j, 128), 128)])

    def third3(self):
        b = self.b
        self.third_y.wait()
        b["ty"][self.y] = b["t_sum"][self.y]
        b["ty_sum"][...] = in_order(b["ty"], 4).astype(BF16)
        self.third_x = Direct(self.links, AX_X, 4, b["tx"])
        self.third_x.start(lambda j: b["ty_sum"])

    def stage3(self):
        b = self.b
        both = b["both"]
        self.first_y.wait()
        own = b["fx_sum"].at[pl.ds(multiple(self.y, 8), 8)]
        slots = [b["fy"].at[lax.rem(self.y + k, 4)] for k in range(1, 4)]
        add_rows(both.at[:, 0], [own] + slots, 8, 8)
        self.second_x.wait()
        own = b["sy_sum"].at[:, :, pl.ds(multiple(self.x, 128), 128)]
        slots = [b["sx"].at[lax.rem(self.x + k, 4)] for k in range(1, 4)]
        add_rows(both.at[:, 1], [own] + slots, 8, 8)
        self.last_z = Direct(self.links, AX_Z, 8, b["lz"])
        self.last_z.start(lambda j: both.at[j])

    def last(self):
        b, t = self.b, self.t
        self.third_x.wait()
        b["tx"][self.x] = b["ty_sum"][...]
        third = in_order(b["tx"], 4)
        self.last_z.wait()
        b["lz"][self.z] = b["both"][self.z]
        piece = in_order(b["lz"], 8)
        b["own"][...] = piece
        b["t_own"][...] = third
        squares = jnp.sum((piece * piece).reshape(4, 8, 128), axis=0)
        return squares + jnp.sum((third * third).reshape(2, 8, 128), axis=0) * 0.25

    def spread(self):
        b, me = self.b, self.x * 2 + self.c
        self.pieces = [self.links.copy(b["t_own"], b["ag_third"].at[self.c], {AX_C: 1 - self.c})]
        for peer in group_peers():
            self.pieces.append(self.links.copy(b["own"], b["ag"].at[me], peer))
        b["ag"][me] = b["own"][...]
        b["ag_third"][self.c] = b["t_own"][...]

    def collect(self, o_first, o_second, o_third):
        b = self.b
        for made in self.pieces:
            made.wait_recv()
        for cc in range(2):
            for xx in range(4):
                me = xx * 2 + cc
                o_first[:, pl.ds(cc * 512 + xx * 128, 128)] = b["ag"][me, 0]
                o_second[pl.ds(cc * 16, 16), pl.ds(xx * 128, 128)] = b["ag"][me, 1]
            o_third[:, pl.ds(cc * 128, 128)] = b["ag_third"][cc]


LINKS = 256


def ring_land(rows, *rest):
    half = pltpu.VMEM((rows // 2, *rest), BF16)
    whole = pltpu.VMEM((rows, *rest), BF16)
    return (half, half, whole, whole)


SUM_BUFS = {
    "a_first": pltpu.VMEM((32, 16, 512), BF16),
    "a_second": pltpu.VMEM((32, 16, 512), BF16),
    "a_third": pltpu.VMEM((4, 8, 16, 128), BF16),
    "fx": ring_land(32, 16, 128),
    "sy": ring_land(8, 16, 512),
    "tz": pltpu.VMEM((8, 4, 16, 128), BF16),
    "t_sum": pltpu.VMEM((4, 16, 128), BF16),
    "ty": pltpu.VMEM((4, 16, 128), BF16),
    "ty_sum": pltpu.VMEM((16, 128), BF16),
    "tx": pltpu.VMEM((4, 16, 128), BF16),
    "fx_sum": pltpu.VMEM((32, 16, 128), BF16),
    "sy_sum": pltpu.VMEM((8, 16, 512), BF16),
    "fy": pltpu.VMEM((4, 8, 16, 128), BF16),
    "sx": pltpu.VMEM((4, 8, 16, 128), BF16),
    "both": pltpu.VMEM((8, 2, 16, 128), BF16),
    "lz": pltpu.VMEM((8, 2, 16, 128), BF16),
    "own": pltpu.VMEM((2, 16, 128), F32),
    "t_own": pltpu.VMEM((16, 128), F32),
    "ag": pltpu.VMEM((8, 2, 16, 128), F32),
    "ag_third": pltpu.VMEM((2, 16, 128), F32),
}

SCALAR_BUFS = {
    "c_in": pltpu.VMEM((8, 8, 128), F32),
    "c_out": pltpu.VMEM((8, 128), F32),
    "p_in": pltpu.VMEM((32, 8, 128), F32),
    "p_out": pltpu.VMEM((8, 128), F32),
    "total": pltpu.VMEM((8, 128), F32),
}


ROWS = pl.ds(0, 4)


class Scalars:
    def __init__(self, links, b):
        self.links, self.b = links, b

    def start(self, squares):
        b, links = self.b, self.links
        me = lax.axis_index(AX_X) * 2 + lax.axis_index(AX_C)
        b["c_out"][0:1] = jnp.sum(squares, axis=0, keepdims=True)
        self.made = [links.copy(b["c_out"].at[ROWS], b["c_in"].at[me, ROWS], peer) for peer in group_peers()]
        b["c_in"][me, ROWS] = b["c_out"][ROWS]

    def over_plane(self):
        b, links = self.b, self.links
        d = lax.axis_index(AX_Y) * 8 + lax.axis_index(AX_Z)
        for made in self.made:
            made.wait_recv()
        b["p_out"][ROWS] = in_order(b["c_in"].at[:, ROWS], 8)
        self.made = [links.copy(b["p_out"].at[ROWS], b["p_in"].at[d, ROWS], peer) for peer in plane_peers()]
        b["p_in"][d, ROWS] = b["p_out"][ROWS]

    def end(self):
        for made in self.made:
            made.wait_recv()
        self.b["total"][ROWS] = in_order(self.b["p_in"].at[:, ROWS], 32)
        return self.b["total"][...]


Q_ROWS, P_ROWS, N_ROWS = pl.ds(0, 256), pl.ds(256, 256), pl.ds(512, 128)
I_ROWS = pl.ds(256, 384)

STEP_BUFS = {
    "pos_ids": pltpu.VMEM((16, 128), jnp.int32),
    "pos_counts": pltpu.VMEM((2, 128), jnp.int32),
    "neg_ids": pltpu.VMEM((16, 128), jnp.int32),
    "neg_counts": pltpu.VMEM((16, 128), jnp.int32),
    "w1": pltpu.VMEM((2, 512, 1024), BF16),
    "w2": pltpu.VMEM((2, 1024, 512), BF16),
    "w3": pltpu.VMEM((2, 512, 256), BF16),
    "x": pltpu.VMEM((640, 512), BF16),
    "a1": pltpu.VMEM((640, 1024), BF16),
    "a2": pltpu.VMEM((640, 512), BF16),
    "s1": pltpu.VMEM((640, 1024), F32),
    "s2": pltpu.VMEM((640, 512), F32),
    "emb": pltpu.VMEM((640, 256), F32),
    "inv": pltpu.VMEM((640, 1), F32),
    "eg": pltpu.VMEM((640, 256), BF16),
    "d2": pltpu.VMEM((640, 512), BF16),
    "d1": pltpu.VMEM((640, 1024), BF16),
    "xt": pltpu.VMEM((512, 640), BF16),
    "a1t": pltpu.VMEM((1024, 640), BF16),
    "a2t": pltpu.VMEM((512, 640), BF16),
    "eye": pltpu.VMEM((256, 256), BF16),
    "pos": pltpu.VMEM((256, 256), BF16),
    "q": pltpu.VMEM((2048, 256), BF16),
    "qs": pltpu.VMEM((2048, 256), BF16),
    "n": pltpu.VMEM((2048, 256), BF16),
    "nt": pltpu.VMEM((256, 2048), BF16),
    "et": pltpu.VMEM((2048, 2048), BF16),
    "turn": pltpu.VMEM((128, 128), F32),
    "ids": pltpu.VMEM((2048, 128), F32),
    "log": pltpu.VMEM((2048, 128), F32),
    "part": pltpu.VMEM((8, 2048), F32),
    "den_out": pltpu.VMEM((16, 128), F32),
    "den_in": pltpu.VMEM((8, 16, 128), F32),
    "den": pltpu.VMEM((16, 128), F32),
    "p_out": pltpu.VMEM((2, 4, 256, 256), BF16),
    "p_pair": pltpu.VMEM((4, 256, 256), BF16),
    "p_ring": ring_land(256, 256),
    "p_sum": pltpu.VMEM((256, 256), F32),
    "g_out": pltpu.VMEM((2048, 256), BF16),
    "g_ring": (ring_land(512, 128), ring_land(512, 128)),
    "g_sum": pltpu.VMEM((2, 512, 128), BF16),
    "g_z": pltpu.VMEM((2, 8, 64, 128), BF16),
    "g_first": pltpu.VMEM((2, 32, 16, 1024), BF16),
    "g_second": pltpu.VMEM((2, 32, 2, 16, 512), BF16),
    "g_third": pltpu.VMEM((2, 4, 8, 16, 256), BF16),
    "sum_query": SUM_BUFS,
    "sum_item": SUM_BUFS,
    "scalars": SCALAR_BUFS,
}


def dot(a, b):
    return jnp.dot(a, b, preferred_element_type=F32)


def dot_cols(a, b):
    return lax.dot_general(a, b, (((1,), (1,)), ((), ())), preferred_element_type=F32)


def silu_both(pre):
    sigma = 0.5 * jnp.tanh(0.5 * pre) + 0.5
    act = pre * sigma
    return act, sigma * (1.0 + pre - act)


def forward(b, t, rows, loads=()):
    def layer(i, carry):
        cols = pl.ds(multiple(i, 512), 512)
        act, slope = silu_both(dot(b["x"][rows, :], b["w1"][t, :, cols]))
        b["a1"][rows, cols] = act.astype(BF16)
        b["s1"][rows, cols] = slope
        return carry

    lax.fori_loop(0, 2, layer, 0, unroll=True)
    for made in loads:
        made.wait()
    act, slope = silu_both(dot(b["a1"][rows, :], b["w2"][t]))
    b["a2"][rows, :] = act.astype(BF16)
    b["s2"][rows, :] = slope
    embedding = dot(b["a2"][rows, :], b["w3"][t])
    inv_norm = lax.rsqrt(jnp.sum(embedding * embedding, axis=1, keepdims=True) + 1.0)
    b["emb"][rows, :] = embedding
    b["inv"][rows, :] = inv_norm
    return (embedding * inv_norm).astype(BF16)


def backward(b, t, rows, unit_grad):
    embedding, inv_norm = b["emb"][rows, :], b["inv"][rows, :]
    along = jnp.sum(embedding * unit_grad, axis=1, keepdims=True)
    embed_grad = inv_norm * unit_grad - inv_norm * inv_norm * inv_norm * embedding * along
    b["eg"][rows, :] = embed_grad.astype(BF16)
    slope = dot_cols(b["eg"][rows, :], b["w3"][t]) * b["s2"][rows, :]
    b["d2"][rows, :] = slope.astype(BF16)

    def layer(i, carry):
        cols = pl.ds(multiple(i, 512), 512)
        slope = dot_cols(b["d2"][rows, :], b["w2"][t, cols, :]) * b["s1"][rows, cols]
        b["d1"][rows, cols] = slope.astype(BF16)
        return carry

    lax.fori_loop(0, 2, layer, 0, unroll=True)


def weight_gradients(b, t, rows, tower):
    def first(i, carry):
        cols = pl.ds(multiple(i, 512), 512)
        made = dot(b["xt"][:, rows], b["d1"][rows, cols]).astype(BF16)
        b["g_first"][t, :, :, cols] = made.reshape(32, 16, 512)
        return carry

    lax.fori_loop(0, 2, first, 0, unroll=True)
    tower.pair_first()

    def second(i, carry):
        at = pl.ds(multiple(i, 512), 512)
        made = dot(b["a1t"][at, rows], b["d2"][rows, :]).astype(BF16)
        b["g_second"][t, pl.ds(multiple(i, 16), 16)] = made.reshape(16, 2, 16, 512)
        return carry

    lax.fori_loop(0, 2, second, 0, unroll=True)
    tower.pair_second()
    third = dot(b["a2t"][:, rows], b["eg"][rows, :]).astype(BF16)
    b["g_third"][t] = third.reshape(4, 8, 16, 256)
    tower.pair_third()


def turn_activations(b, rows):
    for name, cols in (("x", 512), ("a1", 1024), ("a2", 512)):

        def block(i, carry, name=name):
            at = pl.ds(multiple(i, 256), 256)
            turned = dot_cols(b["eye"][...], b[name][rows, at])
            b[name + "t"][at, rows] = turned.astype(BF16)
            return carry

        lax.fori_loop(0, cols // 256, block, 0, unroll=True)


def column(row):
    return jnp.broadcast_to(row, (128, 128)).T


def turn_negatives(b, u):
    for h in range(2):
        half = pl.ds(pl.multiple_of(u * 512 + h * 256, 256), 256)
        b["nt"][:, half] = dot_cols(b["eye"][...], b["n"][half, :]).astype(BF16)


def score_tile(b, pos_ids, u, i):
    at, cols = pl.ds(multiple(u, 512), 512), pl.ds(multiple(i, 512), 512)
    products = dot_cols(b["n"][at, :], b["q"][cols, :])
    logs = jnp.concatenate([b["log"][at, :]] * 4, axis=1)
    ids = jnp.concatenate([b["ids"][at, :]] * 4, axis=1)
    weights = jnp.exp2(products * (inv_temp * LOG2_E) - logs)
    rows = [pos_ids[pl.ds(i * 4 + r, 1), :].astype(F32) for r in range(4)]
    weights = jnp.where(jnp.concatenate(rows, axis=1) != ids, weights, 0.0)
    b["et"][at, cols] = weights.astype(BF16)
    b["part"][:, cols] += jnp.sum(weights.reshape(64, 8, 512), axis=0)


def step_kernel(
    query_x,
    positive_x,
    negative_x,
    q1,
    q2,
    q3,
    i1,
    i2,
    i3,
    pos_ids_in,
    pos_counts_in,
    neg_ids_in,
    neg_counts_in,
    o_query_first,
    o_query_second,
    o_query_third,
    o_item_first,
    o_item_second,
    o_item_third,
    o_scalars,
    b,
    load,
    send,
    recv,
):
    y, z, x, c = (lax.axis_index(a) for a in (AX_Y, AX_Z, AX_X, AX_C))
    me = x * 2 + c
    links = Links(send, recv, LINKS)
    phase = Phases()

    loads = [
        (negative_x, b["x"].at[pl.ds(512, 64)]),
        (i1, b["w1"].at[1]),
        (i2, b["w2"].at[1]),
        (i3, b["w3"].at[1]),
        (query_x, b["x"].at[Q_ROWS]),
        (q1, b["w1"].at[0]),
        (q2, b["w2"].at[0]),
        (q3, b["w3"].at[0]),
        (positive_x, b["x"].at[P_ROWS]),
        (pos_ids_in, b["pos_ids"]),
        (pos_counts_in, b["pos_counts"]),
        (neg_ids_in, b["neg_ids"]),
        (neg_counts_in, b["neg_counts"]),
    ]
    loads = [pltpu.make_async_copy(s, d, load.at[k]) for k, (s, d) in enumerate(loads)]
    for made in loads[:4]:
        made.start()
    barrier, peers = greet_neighbours()
    phase("load")
    for made in loads[4:]:
        made.start()

    b["x"][pl.ds(576, 64), :] = jnp.zeros((64, 512), BF16)
    b["part"][...] = jnp.zeros((8, 2048), F32)
    b["scalars"]["c_out"][...] = jnp.zeros((8, 128), F32)
    b["scalars"]["total"][...] = jnp.zeros((8, 128), F32)
    ones = lax.broadcasted_iota(jnp.int32, (256, 256), 0) == lax.broadcasted_iota(
        jnp.int32, (256, 256), 1
    )
    b["eye"][...] = jnp.where(ones, 1.0, 0.0).astype(BF16)

    loads[0].wait()
    loads[1].wait()
    phase("f_neg")
    n = b["n"]
    unit = forward(b, 1, N_ROWS, loads[2:4])

    def n_block(yy, zz):
        return n.at[pl.ds(pl.multiple_of((yy * 8 + zz) * 64, 64), 64)]

    def n_half(yy, zz, h):
        return n.at[pl.ds(pl.multiple_of((yy * 8 + zz) * 64 + h * 32, 32), 32)]

    n[pl.ds(pl.multiple_of((y * 8 + z) * 64, 64), 64), :] = unit[:64]
    phase("barrier")
    pl.semaphore_wait(barrier, peers)
    y_up, y_down = lax.rem(y + 1, 4), lax.rem(y + 3, 4)
    order = (1, 7, 2, 6, 3, 5, 4)
    n_z, n_y = {}, {}
    for k in order:
        n_z[k] = links.copy(n_block(y, z), n_block(y, z), {AX_Z: lax.rem(z + k, 8)})

    def n_forward(k):
        zz = lax.rem(z - k + 8, 8)
        n_y[k] = (
            links.copy(n_block(y, zz), n_block(y, zz), {AX_Y: y_up}),
            links.copy(n_block(y, zz), n_block(y, zz), {AX_Y: y_down}),
        )

    n_forward(0)

    phase("f_query")
    for made in loads[4:8]:
        made.wait()
    q = b["q"]
    q_own = forward(b, 0, Q_ROWS)

    def q_block(xx, cc):
        return q.at[pl.ds(pl.multiple_of((xx * 2 + cc) * 256, 256), 256)]

    def q_half(xx, cc, h):
        return q.at[pl.ds(pl.multiple_of((xx * 2 + cc) * 256 + h * 128, 128), 128)]

    q[pl.ds(multiple(me, 256), 256), :] = q_own
    x_up, x_down, x_far = lax.rem(x + 1, 4), lax.rem(x + 3, 4), lax.rem(x + 2, 4)
    other = {AX_C: 1 - c}
    q_up, q_down = {}, {}
    for h in range(2):
        q_up[h] = links.copy(q_half(x, c, h), q_half(x, c, h), {AX_X: x_up})
        q_down[1 - h] = links.copy(q_half(x, c, 1 - h), q_half(x, c, 1 - h), {AX_X: x_down})
    q_pair = [links.copy(q_block(x, c), q_block(x, c), other)]

    phase("f_pos")
    for made in loads[8:]:
        made.wait()
    pos_ids, pos_counts, neg_ids, neg_counts = (
        b[k] for k in ("pos_ids", "pos_counts", "neg_ids", "neg_counts")
    )
    b["pos"][...] = forward(b, 1, P_ROWS)

    phase("n_fwd1")
    for k in order[:4]:
        n_z[k].wait_recv()
        n_forward(k)
    phase("q_relay")
    q_up[0].wait_recv()
    q_low = links.copy(q_half(x_down, c, 0), q_half(x_down, c, 0), {AX_X: x_up})
    q_down[1].wait_recv()
    q_high = links.copy(q_half(x_up, c, 1), q_half(x_up, c, 1), {AX_X: x_down})
    q_up[1].wait_recv()
    q_pair.append(links.copy(q_block(x_down, c), q_block(x_down, c), other))
    q_down[0].wait_recv()
    q_pair.append(links.copy(q_block(x_up, c), q_block(x_up, c), other))

    phase("small")
    turn = b["turn"]
    turn[...] = jnp.zeros((128, 128), F32)
    turn[pl.ds(0, 16), :] = neg_ids[...].astype(F32)
    turn[pl.ds(16, 16), :] = jnp.log(neg_counts[...].astype(F32)) * LOG2_E
    turned = turn[...].T
    for j in range(16):
        b["ids"][pl.ds(j * 128, 128), :] = jnp.broadcast_to(turned[:, j : j + 1], (128, 128))
        b["log"][pl.ds(j * 128, 128), :] = jnp.broadcast_to(
            turned[:, 16 + j : 17 + j], (128, 128)
        )
    phase("n_fwd2")
    for k in order[4:]:
        n_z[k].wait_recv()
        n_forward(k)

    n_far = []

    def n_relay(*which):
        for k in which:
            zz = lax.rem(z - k + 8, 8)
            from_down, from_up = n_y[k]
            from_down.wait_recv()
            n_far.append(
                links.copy(n_half(y_down, zz, 0), n_half(y_down, zz, 0), {AX_Y: y_up})
            )
            from_up.wait_recv()
            n_far.append(
                links.copy(n_half(y_up, zz, 1), n_half(y_up, zz, 1), {AX_Y: y_down})
            )

    phase("relay_a")
    n_relay(0, 1, 7)
    q_pair[0].wait_recv()
    phase("tile_a")
    score_tile(b, pos_ids, y, x)
    phase("relay_b")
    n_relay(2, 6)
    q_pair[1].wait_recv()
    phase("tile_b")
    score_tile(b, pos_ids, y, x_down)
    phase("relay_c")
    q_low.wait_recv()
    q_pair.append(links.copy(q_half(x_far, c, 0), q_half(x_far, c, 0), other))
    q_high.wait_recv()
    q_pair.append(links.copy(q_half(x_far, c, 1), q_half(x_far, c, 1), other))
    n_relay(3, 5)
    q_pair[2].wait_recv()
    phase("tile_c")
    score_tile(b, pos_ids, y, x_up)
    phase("relay_d")
    n_relay(4)
    phase("tiles")
    for made in q_pair[3:]:
        made.wait_recv()
    score_tile(b, pos_ids, y, x_far)

    def near_tiles(i, carry):
        score_tile(b, pos_ids, y_up, i)
        score_tile(b, pos_ids, y_down, i)
        return carry

    lax.fori_loop(0, 4, near_tiles, 0)
    phase("logits")
    own = b["q"][pl.ds(multiple(me, 256), 256), :].astype(F32)
    along = jnp.sum(own * b["pos"][...].astype(F32), axis=1, keepdims=True)
    logits = []
    for h in range(2):
        row = jnp.broadcast_to(along[h * 128 : (h + 1) * 128], (128, 128)).T[0:1, :]
        logits.append(row * inv_temp - jnp.log(pos_counts[h : h + 1, :].astype(F32)))

    phase("n_far")
    for made in n_far:
        made.wait_recv()
    phase("far_tiles")
    y_far = lax.rem(y + 2, 4)

    def far_tiles(i, carry):
        score_tile(b, pos_ids, y_far, i)
        return carry

    lax.fori_loop(0, 4, far_tiles, 0, unroll=2)

    phase("den")
    den_out, den_in = b["den_out"], b["den_in"]
    for j in range(16):
        den_out[pl.ds(j, 1), :] = jnp.sum(b["part"][:, j * 128 : (j + 1) * 128], axis=0, keepdims=True)
    for h in range(2):
        at = pl.ds(me * 2 + h, 1)
        den_out[at, :] = den_out[at, :] + jnp.exp(logits[h])
    sums = [links.copy(den_out, den_in.at[me], peer) for peer in group_peers()]
    den_in[me] = den_out[...]

    def turned(u, carry):
        turn_negatives(b, u)
        return carry

    lax.fori_loop(0, 4, turned, 0, unroll=True)

    phase("p_theirs")
    p_out = b["p_out"]

    def query_block(cc, i):
        cols = pl.ds(pl.multiple_of((i * 2 + cc) * 256, 256), 256)
        p_out[cc, i] = dot(b["nt"][...], b["et"][:, cols]).astype(BF16)

    def theirs(i, carry):
        query_block(1 - c, i)
        return carry

    def ours(i, carry):
        query_block(c, i)
        return carry

    lax.fori_loop(0, 4, theirs, 0, unroll=2)
    p_pair = b["p_pair"]
    pair = links.copy(p_out.at[1 - c], p_pair, other)
    phase("p_ours")
    lax.fori_loop(0, 4, ours, 0, unroll=2)
    phase("p_add")
    pair.wait_recv()
    for i in range(4):
        add_rows(p_pair.at[i], (p_pair.at[i], p_out.at[c, i]), 256, 64)
    p_x = Ring4(links, AX_X, lambda j: p_pair.at[j], 256, b["p_ring"], 128)
    p_x.start()

    phase("den_wait")
    for made in sums:
        made.wait_recv()
    total = in_order(den_in, 8)
    b["den"][...] = total
    turn[pl.ds(0, 16), :] = 1.0 / total
    turned = turn[...].T
    for j in range(16):
        at = pl.ds(j * 128, 128)
        b["qs"][at, :] = (q[at, :].astype(F32) * turned[:, j : j + 1]).astype(BF16)

    phase("g_rows")
    g_out = b["g_out"]

    def negative_rows(u):
        at = pl.ds(multiple(u, 512), 512)
        g_out[at, :] = dot(b["et"][at, :], b["qs"][...]).astype(BF16)

    g_y, g_z, g_sum = [], [], b["g_sum"]
    for h in range(2):
        cols = pl.ds(h * 128, 128)

        def cut(j, cols=cols):
            return g_out.at[pl.ds(multiple(j, 512), 512), cols]

        g_y.append(Ring4(links, AX_Y, cut, 512, b["g_ring"][h], 64))
        g_z.append(Direct(links, AX_Z, 8, b["g_z"].at[h]))
    negative_rows(g_y[0].far)
    g_y[0].start_far()
    g_y[1].start_far()
    negative_rows(g_y[0].up)
    negative_rows(g_y[0].down)
    g_y[0].start_near()

    def g_line(h):
        g_y[h].end(g_sum.at[h])
        g_z[h].start(lambda j: g_sum.at[h, pl.ds(multiple(j, 64), 64)])
    phase("p_relay")
    p_x.relay()
    phase("g_own")
    negative_rows(g_y[0].me)
    phase("g_relay0")
    g_y[0].relay()
    g_y[1].start_near()

    phase("slopes")
    losses, slopes, scales = [], [], []
    for h in range(2):
        den = b["den"][pl.ds(me * 2 + h, 1), :]
        losses.append(jnp.log(den) - logits[h])
        slope = column(jnp.exp(logits[h]) / den - 1.0) * inv_temp
        slopes.append(jnp.concatenate([slope, slope], axis=1))
        scale = column(inv_temp / den)
        scales.append(jnp.concatenate([scale, scale], axis=1))
    slopes = jnp.concatenate(slopes, axis=0)
    scales = jnp.concatenate(scales, axis=0)
    for h in range(2):
        b["scalars"]["c_out"][h + 1 : h + 2] = losses[h]
    phase("b_pos")
    own = q[pl.ds(multiple(me, 256), 256), :].astype(F32)
    backward(b, 1, P_ROWS, slopes * own)
    phase("g_relay1")
    g_y[1].relay()
    phase("turn_q")
    turn_activations(b, Q_ROWS)

    phase("p_end")
    p_x.end(b["p_sum"])
    query_grad = b["p_sum"][...].T * scales + slopes * b["pos"][...].astype(F32)
    phase("b_query")
    backward(b, 0, Q_ROWS, query_grad)
    phase("g_end0")
    g_line(0)
    phase("w_query")
    query_sum = TowerSum(links, b["sum_query"], b, 0)
    item_sum = TowerSum(links, b["sum_item"], b, 1)
    weight_gradients(b, 0, Q_ROWS, query_sum)
    phase("g_end1")
    g_line(1)

    phase("turn_n")
    turn_activations(b, N_ROWS)
    phase("q_stage1")
    query_sum.stage1()
    phase("turn_p")
    turn_activations(b, P_ROWS)
    phase("q_relay1")
    query_sum.relay1()

    phase("g_z")
    halves = []
    for h in range(2):
        g_z[h].wait()
        total = g_sum[h, pl.ds(multiple(z, 64), 64), :].astype(F32)
        for k in range(1, 8):
            total = total + b["g_z"][h, lax.rem(z + k, 8)].astype(F32)
        halves.append(total)
    total = jnp.concatenate(halves, axis=1)
    total = jnp.concatenate([total * inv_temp, jnp.zeros((64, 256), F32)], axis=0)
    phase("b_neg")
    backward(b, 1, N_ROWS, total)
    phase("w_item")
    weight_gradients(b, 1, I_ROWS, item_sum)
    phase("i_stage1")
    item_sum.stage1()
    phase("q_stage2")
    query_sum.stage2()
    query_sum.third1()
    item_sum.third1()
    phase("i_relay1")
    item_sum.relay1()
    phase("q_stage3")
    query_sum.stage3()
    query_sum.third2()
    phase("i_stage2")
    item_sum.stage2()
    phase("q_third3")
    query_sum.third3()
    item_sum.third2()
    phase("i_stage3")
    item_sum.stage3()
    phase("q_last")
    item_sum.third3()
    squares = query_sum.last()
    query_sum.spread()
    phase("i_last")
    squares = squares + item_sum.last()
    scalars = Scalars(links, b["scalars"])
    scalars.start(squares)
    phase("group")
    scalars.over_plane()
    item_sum.spread()
    phase("plane")
    total = scalars.end()
    row = lax.broadcasted_iota(jnp.int32, (8, 128), 0)
    norm = jnp.sqrt(jnp.sum(jnp.where(row == 0, total, 0.0), keepdims=True))
    factor = clip_norm / jnp.maximum(norm, clip_norm)
    o_scalars[0] = jnp.broadcast_to(factor, (8, 128))
    o_scalars[1] = jnp.broadcast_to(jnp.sum(jnp.where((row == 1) | (row == 2), total, 0.0), keepdims=True), (8, 128))
    phase("pieces")
    query_sum.collect(o_query_first, o_query_second, o_query_third)
    item_sum.collect(o_item_first, o_item_second, o_item_third)
    phase("finish")
    links.finish()
    phase(None)


def clip_kernel(*refs):
    scalars, raw, clipped, loss = refs[0], refs[1:7], refs[7:13], refs[13]
    factor = scalars[0, 0:1, 0:1]
    for source, result in zip(raw, clipped):
        result[...] = source[...] * factor
    loss[...] = scalars[1, 0:1, 0:1] * (1.0 / QUERIES)


def per_device(
    query_features,
    positive_features,
    negative_features,
    positive_ids,
    positive_counts,
    negative_ids,
    negative_counts,
    query_first,
    query_second,
    query_third,
    item_first,
    item_second,
    item_third,
):
    vmem = pl.BlockSpec(memory_space=pltpu.VMEM)
    anywhere = pl.BlockSpec(memory_space=pl.ANY)
    tower = (
        jax.ShapeDtypeStruct((16, 1024), F32),
        jax.ShapeDtypeStruct((32, 512), F32),
        jax.ShapeDtypeStruct((16, 256), F32),
    )
    *raw, scalars = pl.pallas_call(
        step_kernel,
        out_shape=tower + tower + (jax.ShapeDtypeStruct((2, 8, 128), F32),),
        in_specs=[anywhere] * 13,
        out_specs=(vmem,) * 7,
        scratch_shapes=[
            STEP_BUFS,
            pltpu.SemaphoreType.DMA((13,)),
            pltpu.SemaphoreType.DMA((LINKS,)),
            pltpu.SemaphoreType.DMA((LINKS,)),
        ],
        compiler_params=pltpu.CompilerParams(
            collective_id=0, has_side_effects=True, vmem_limit_bytes=56 * 1024 * 1024
        ),
        name="training_step",
    )(
        query_features,
        positive_features,
        negative_features,
        query_first,
        query_second,
        query_third,
        item_first,
        item_second,
        item_third,
        positive_ids.reshape(16, 128),
        positive_counts.reshape(2, 128),
        negative_ids.reshape(16, 128),
        negative_counts.reshape(16, 128),
    )
    *clipped, loss = pl.pallas_call(
        clip_kernel,
        out_shape=tower + tower + (jax.ShapeDtypeStruct((1, 1), F32),),
        in_specs=[vmem] * 7,
        out_specs=(vmem,) * 7,
        name="clip",
    )(scalars, *raw)
    return (loss.reshape(()), *clipped)


def solution(mesh):
    torus = Mesh(mesh.devices.reshape(4, 8, 4, 2), DP_NEG)
    placed = (
        P(DP_NEG, None),
        P(DP_NEG, None),
        P(NEG_DP, None),
        P(DP),
        P(DP_NEG),
        P(NEG),
        P(NEG),
        P(),
        P(),
        P(),
        P(),
        P(),
        P(),
    )
    return jax.shard_map(
        per_device,
        mesh=torus,
        in_specs=placed,
        out_specs=(P(),) + (P(DP, None),) * 6,
        check_vma=False,
    )
```

```python
import jax
import jax.numpy as jnp
from jax import lax
from jax.experimental import pallas as pl
from jax.experimental.pallas import tpu as pltpu
from jax.sharding import Mesh
from jax.sharding import PartitionSpec as P

NEG = ("neg_0", "neg_1")
DP = ("dp_0", "dp_1")
DP_NEG = ("dp_0", "dp_1", "neg_0", "neg_1")
NEG_DP = ("neg_0", "neg_1", "dp_0", "dp_1")
AX_Y, AX_Z, AX_X, AX_C = "dp_0", "dp_1", "neg_0", "neg_1"
MESH = pl.DeviceIdType.MESH
F32 = jnp.float32
BF16 = jnp.bfloat16

QUERIES = 65536
inv_temp = 20.0
clip_norm = 256.0
LOG2_E = 1.4426950408889634


class Links:
    def __init__(self, send_sems, recv_sems, size):
        self.send_sems, self.recv_sems, self.size = send_sems, recv_sems, size
        self.used = 0
        self.started = []

    def copy(self, src, dst, device):
        at = self.used
        self.used += 1
        assert at < self.size
        made = pltpu.make_async_remote_copy(
            src_ref=src,
            dst_ref=dst,
            send_sem=self.send_sems.at[at],
            recv_sem=self.recv_sems.at[at],
            device_id=device,
            device_id_type=MESH,
        )
        made.start()
        self.started.append(made)
        return made

    def finish(self):
        for made in self.started:
            made.wait_send()


def add_rows(out, terms, rows, step):
    def body(i, carry):
        at = pl.ds(pl.multiple_of(i * step, step), step)
        total = terms[0][at].astype(F32)
        for term in terms[1:]:
            total = total + term[at].astype(F32)
        out[at] = total.astype(out.dtype)
        return carry

    if rows == step:
        body(0, 0)
    else:
        lax.fori_loop(0, rows // step, body, 0)


class Phases:
    def __init__(self):
        self.scope = None

    def __call__(self, name):
        if self.scope is not None:
            self.scope.__exit__(None, None, None)
        self.scope = None
        if name is not None:
            self.scope = jax.named_scope(name)
            self.scope.__enter__()


class Ring4:
    def __init__(self, links, axis, cut, rows, land, step):
        self.links, self.axis, self.cut, self.rows, self.step = links, axis, cut, rows, step
        self.early_up, self.early_down, self.from_down, self.from_up = land
        me = lax.axis_index(axis)
        self.me = me
        self.up, self.down, self.far = lax.rem(me + 1, 4), lax.rem(me + 3, 4), lax.rem(me + 2, 4)
        half = rows // 2
        self.half, self.low, self.high = half, pl.ds(0, half), pl.ds(half, half)

    def start_far(self):
        far = self.cut(self.far)
        self.a = self.links.copy(far.at[self.low], self.early_up, {self.axis: self.up})
        self.b = self.links.copy(far.at[self.high], self.early_down, {self.axis: self.down})

    def start_near(self):
        self.start_up()
        self.start_down()

    def start_up(self):
        self.c = self.links.copy(
            self.cut(self.up).at[self.high], self.from_down.at[self.high], {self.axis: self.up}
        )

    def start_down(self):
        self.d = self.links.copy(
            self.cut(self.down).at[self.low], self.from_up.at[self.low], {self.axis: self.down}
        )

    def start(self):
        self.start_far()
        self.start_near()

    def relay(self):
        self.a.wait_recv()
        mine = self.cut(self.up).at[self.low]
        add_rows(self.early_up, (mine, self.early_up), self.half, self.step)
        self.e = self.links.copy(self.early_up, self.from_down.at[self.low], {self.axis: self.up})
        self.b.wait_recv()
        mine = self.cut(self.down).at[self.high]
        add_rows(self.early_down, (mine, self.early_down), self.half, self.step)
        self.f = self.links.copy(
            self.early_down, self.from_up.at[self.high], {self.axis: self.down}
        )

    def end(self, out):
        for made in (self.c, self.d, self.e, self.f):
            made.wait_recv()
        add_rows(out, (self.cut(self.me), self.from_down, self.from_up), self.rows, self.step)


class Direct:
    def __init__(self, links, axis, size, slots):
        self.links, self.axis, self.size, self.slots = links, axis, size, slots
        self.me = lax.axis_index(axis)

    def start(self, cut):
        self.made = []
        for k in range(1, self.size):
            to = lax.rem(self.me + k, self.size)
            self.made.append(self.links.copy(cut(to), self.slots.at[self.me], {self.axis: to}))

    def wait(self):
        for made in self.made:
            made.wait_recv()


def in_order(slots, count):
    total = slots[0].astype(F32)
    for j in range(1, count):
        total = total + slots[j].astype(F32)
    return total


def group_peers():
    x, c = lax.axis_index(AX_X), lax.axis_index(AX_C)
    peers = []
    for k in range(1, 8):
        other = lax.rem(x * 2 + c + k, 8)
        peers.append({AX_X: other // 2, AX_C: lax.rem(other, 2)})
    return peers


def plane_peers():
    y, z = lax.axis_index(AX_Y), lax.axis_index(AX_Z)
    peers = []
    for k in range(1, 32):
        other = lax.rem(y * 8 + z + k, 32)
        peers.append({AX_Y: other // 8, AX_Z: lax.rem(other, 8)})
    return peers


def greet_neighbours():
    barrier = pltpu.get_barrier_semaphore()
    peers = group_peers() + plane_peers()
    for peer in peers:
        pl.semaphore_signal(barrier, inc=1, device_id=peer, device_id_type=MESH)
    return barrier, len(peers)


def multiple(index, size):
    return pl.multiple_of(index * size, size)


class TowerSum:
    def __init__(self, links, b, g, t):
        self.links, self.b, self.t, self.g = links, b, t, g
        self.y, self.z, self.x, self.c = (lax.axis_index(a) for a in (AX_Y, AX_Z, AX_X, AX_C))

    def pair_first(self):
        columns = pl.ds(multiple(1 - self.c, 512), 512)
        mine = self.g["g_first"].at[self.t, :, :, columns]
        self.pair = [self.links.copy(mine, self.b["a_first"], {AX_C: 1 - self.c})]

    def pair_second(self):
        mine = self.g["g_second"].at[self.t, :, 1 - self.c]
        self.pair.append(self.links.copy(mine, self.b["a_second"], {AX_C: 1 - self.c}))

    def pair_third(self):
        columns = pl.ds(multiple(1 - self.c, 128), 128)
        mine = self.g["g_third"].at[self.t, :, :, :, columns]
        self.pair.append(self.links.copy(mine, self.b["a_third"], {AX_C: 1 - self.c}))

    def stage1(self):
        t, c, g, b, links = self.t, self.c, self.g, self.b, self.links
        first, second = b["a_first"], b["a_second"]
        self.pair[0].wait_recv()
        own = g["g_first"].at[t, :, :, pl.ds(multiple(c, 512), 512)]
        add_rows(first, (first, own), 32, 4)
        self.first_x = Ring4(
            links, AX_X, lambda j: first.at[:, :, pl.ds(multiple(j, 128), 128)], 32, b["fx"], 16
        )
        self.first_x.start()
        self.pair[1].wait_recv()
        add_rows(second, (second, g["g_second"].at[t, :, c]), 32, 4)
        self.second_y = Ring4(
            links, AX_Y, lambda j: second.at[pl.ds(multiple(j, 8), 8)], 8, b["sy"], 4
        )
        self.second_y.start()

    def third1(self):
        t, c, g, b, links = self.t, self.c, self.g, self.b, self.links
        third = b["a_third"]
        self.pair[2].wait_recv()
        own = g["g_third"].at[t, :, :, :, pl.ds(multiple(c, 128), 128)]
        add_rows(third, (third, own), 4, 1)
        self.third_z = Direct(links, AX_Z, 8, b["tz"])
        self.third_z.start(lambda j: third.at[:, j])

    def relay1(self):
        self.first_x.relay()
        self.second_y.relay()

    def third2(self):
        b = self.b
        self.third_z.wait()
        b["tz"][self.z] = b["a_third"][:, self.z]
        b["t_sum"][...] = in_order(b["tz"], 8).astype(BF16)
        self.third_y = Direct(self.links, AX_Y, 4, b["ty"])
        self.third_y.start(lambda j: b["t_sum"].at[j])

    def stage2(self):
        b, links = self.b, self.links
        fx_sum, sy_sum = b["fx_sum"], b["sy_sum"]
        self.first_x.end(fx_sum)
        self.first_y = Direct(links, AX_Y, 4, b["fy"])
        self.first_y.start(lambda j: fx_sum.at[pl.ds(multiple(j, 8), 8)])
        self.second_y.end(sy_sum)
        self.second_x = Direct(links, AX_X, 4, b["sx"])
        self.second_x.start(lambda j: sy_sum.at[:, :, pl.ds(multiple(j, 128), 128)])

    def third3(self):
        b = self.b
        self.third_y.wait()
        b["ty"][self.y] = b["t_sum"][self.y]
        b["ty_sum"][...] = in_order(b["ty"], 4).astype(BF16)
        self.third_x = Direct(self.links, AX_X, 4, b["tx"])
        self.third_x.start(lambda j: b["ty_sum"])

    def stage3(self):
        b = self.b
        both = b["both"]
        self.first_y.wait()
        own = b["fx_sum"].at[pl.ds(multiple(self.y, 8), 8)]
        slots = [b["fy"].at[lax.rem(self.y + k, 4)] for k in range(1, 4)]
        add_rows(both.at[:, 0], [own] + slots, 8, 8)
        self.second_x.wait()
        own = b["sy_sum"].at[:, :, pl.ds(multiple(self.x, 128), 128)]
        slots = [b["sx"].at[lax.rem(self.x + k, 4)] for k in range(1, 4)]
        add_rows(both.at[:, 1], [own] + slots, 8, 8)
        self.last_z = Direct(self.links, AX_Z, 8, b["lz"])
        self.last_z.start(lambda j: both.at[j])

    def last(self):
        b, t = self.b, self.t
        self.third_x.wait()
        b["tx"][self.x] = b["ty_sum"][...]
        third = in_order(b["tx"], 4)
        self.last_z.wait()
        b["lz"][self.z] = b["both"][self.z]
        piece = in_order(b["lz"], 8)
        b["own"][...] = piece
        b["t_own"][...] = third
        squares = jnp.sum((piece * piece).reshape(4, 8, 128), axis=0)
        return squares + jnp.sum((third * third).reshape(2, 8, 128), axis=0) * 0.25

    def spread(self):
        b, me = self.b, self.x * 2 + self.c
        self.pieces = [self.links.copy(b["t_own"], b["ag_third"].at[self.c], {AX_C: 1 - self.c})]
        for peer in group_peers():
            self.pieces.append(self.links.copy(b["own"], b["ag"].at[me], peer))
        b["ag"][me] = b["own"][...]
        b["ag_third"][self.c] = b["t_own"][...]

    def collect(self, o_first, o_second, o_third):
        b = self.b
        for made in self.pieces:
            made.wait_recv()
        for cc in range(2):
            for xx in range(4):
                me = xx * 2 + cc
                o_first[:, pl.ds(cc * 512 + xx * 128, 128)] = b["ag"][me, 0]
                o_second[pl.ds(cc * 16, 16), pl.ds(xx * 128, 128)] = b["ag"][me, 1]
            o_third[:, pl.ds(cc * 128, 128)] = b["ag_third"][cc]


LINKS = 256


def ring_land(rows, *rest):
    half = pltpu.VMEM((rows // 2, *rest), BF16)
    whole = pltpu.VMEM((rows, *rest), BF16)
    return (half, half, whole, whole)


SUM_BUFS = {
    "a_first": pltpu.VMEM((32, 16, 512), BF16),
    "a_second": pltpu.VMEM((32, 16, 512), BF16),
    "a_third": pltpu.VMEM((4, 8, 16, 128), BF16),
    "fx": ring_land(32, 16, 128),
    "sy": ring_land(8, 16, 512),
    "tz": pltpu.VMEM((8, 4, 16, 128), BF16),
    "t_sum": pltpu.VMEM((4, 16, 128), BF16),
    "ty": pltpu.VMEM((4, 16, 128), BF16),
    "ty_sum": pltpu.VMEM((16, 128), BF16),
    "tx": pltpu.VMEM((4, 16, 128), BF16),
    "fx_sum": pltpu.VMEM((32, 16, 128), BF16),
    "sy_sum": pltpu.VMEM((8, 16, 512), BF16),
    "fy": pltpu.VMEM((4, 8, 16, 128), BF16),
    "sx": pltpu.VMEM((4, 8, 16, 128), BF16),
    "both": pltpu.VMEM((8, 2, 16, 128), BF16),
    "lz": pltpu.VMEM((8, 2, 16, 128), BF16),
    "own": pltpu.VMEM((2, 16, 128), F32),
    "t_own": pltpu.VMEM((16, 128), F32),
    "ag": pltpu.VMEM((8, 2, 16, 128), F32),
    "ag_third": pltpu.VMEM((2, 16, 128), F32),
}

SCALAR_BUFS = {
    "c_in": pltpu.VMEM((8, 8, 128), F32),
    "c_out": pltpu.VMEM((8, 128), F32),
    "p_in": pltpu.VMEM((32, 8, 128), F32),
    "p_out": pltpu.VMEM((8, 128), F32),
    "total": pltpu.VMEM((8, 128), F32),
}


ROWS = pl.ds(0, 4)


class Scalars:
    def __init__(self, links, b):
        self.links, self.b = links, b

    def start(self, squares):
        b, links = self.b, self.links
        me = lax.axis_index(AX_X) * 2 + lax.axis_index(AX_C)
        b["c_out"][0:1] = jnp.sum(squares, axis=0, keepdims=True)
        self.made = [links.copy(b["c_out"].at[ROWS], b["c_in"].at[me, ROWS], peer) for peer in group_peers()]
        b["c_in"][me, ROWS] = b["c_out"][ROWS]

    def over_plane(self):
        b, links = self.b, self.links
        d = lax.axis_index(AX_Y) * 8 + lax.axis_index(AX_Z)
        for made in self.made:
            made.wait_recv()
        b["p_out"][ROWS] = in_order(b["c_in"].at[:, ROWS], 8)
        self.made = [links.copy(b["p_out"].at[ROWS], b["p_in"].at[d, ROWS], peer) for peer in plane_peers()]
        b["p_in"][d, ROWS] = b["p_out"][ROWS]

    def end(self):
        for made in self.made:
            made.wait_recv()
        self.b["total"][ROWS] = in_order(self.b["p_in"].at[:, ROWS], 32)
        return self.b["total"][...]


Q_ROWS, P_ROWS, N_ROWS = pl.ds(0, 256), pl.ds(256, 256), pl.ds(512, 128)

STEP_BUFS = {
    "pos_ids": pltpu.VMEM((16, 128), jnp.int32),
    "pos_counts": pltpu.VMEM((2, 128), jnp.int32),
    "neg_ids": pltpu.VMEM((16, 128), jnp.int32),
    "neg_counts": pltpu.VMEM((16, 128), jnp.int32),
    "w1": pltpu.VMEM((2, 512, 1024), BF16),
    "w2": pltpu.VMEM((2, 1024, 512), BF16),
    "w3": pltpu.VMEM((2, 512, 256), BF16),
    "x": pltpu.VMEM((640, 512), BF16),
    "a1": pltpu.VMEM((640, 1024), BF16),
    "a2": pltpu.VMEM((640, 512), BF16),
    "s1": pltpu.VMEM((640, 1024), F32),
    "s2": pltpu.VMEM((640, 512), F32),
    "emb": pltpu.VMEM((640, 256), F32),
    "inv": pltpu.VMEM((640, 1), F32),
    "eg": pltpu.VMEM((640, 256), BF16),
    "d2": pltpu.VMEM((640, 512), BF16),
    "d1": pltpu.VMEM((640, 1024), BF16),
    "xt": pltpu.VMEM((512, 640), BF16),
    "a1t": pltpu.VMEM((1024, 640), BF16),
    "a2t": pltpu.VMEM((512, 640), BF16),
    "eye": pltpu.VMEM((256, 256), BF16),
    "pos": pltpu.VMEM((256, 256), BF16),
    "q": pltpu.VMEM((2048, 256), BF16),
    "qs": pltpu.VMEM((2048, 256), BF16),
    "n": pltpu.VMEM((2048, 256), BF16),
    "nt": pltpu.VMEM((256, 2048), BF16),
    "et": pltpu.VMEM((2048, 2048), BF16),
    "turn": pltpu.VMEM((128, 128), F32),
    "ids": pltpu.VMEM((2048, 128), F32),
    "log": pltpu.VMEM((2048, 128), F32),
    "part": pltpu.VMEM((8, 2048), F32),
    "den_out": pltpu.VMEM((16, 128), F32),
    "den_in": pltpu.VMEM((8, 16, 128), F32),
    "den": pltpu.VMEM((16, 128), F32),
    "p_out": pltpu.VMEM((2, 4, 256, 256), BF16),
    "p_pair": pltpu.VMEM((4, 256, 256), BF16),
    "p_ring": ring_land(256, 256),
    "p_sum": pltpu.VMEM((256, 256), F32),
    "g_out": pltpu.VMEM((2048, 256), BF16),
    "g_ring": (ring_land(512, 128), ring_land(512, 128)),
    "g_sum": pltpu.VMEM((2, 512, 128), BF16),
    "g_z": pltpu.VMEM((2, 8, 64, 128), BF16),
    "g_first": pltpu.VMEM((2, 32, 16, 1024), BF16),
    "g_second": pltpu.VMEM((2, 32, 2, 16, 512), BF16),
    "g_third": pltpu.VMEM((2, 4, 8, 16, 256), BF16),
    "kept_first": pltpu.VMEM((512, 1024), F32),
    "kept_second": pltpu.VMEM((1024, 512), F32),
    "kept_third": pltpu.VMEM((512, 256), F32),
    "stage": tuple(pltpu.VMEM(shape, F32) for shape in ((16, 1024), (32, 512), (16, 256)) * 2),
    "sum_query": SUM_BUFS,
    "sum_item": SUM_BUFS,
    "scalars": SCALAR_BUFS,
}


def dot(a, b):
    return jnp.dot(a, b, preferred_element_type=F32)


def dot_cols(a, b):
    return lax.dot_general(a, b, (((1,), (1,)), ((), ())), preferred_element_type=F32)


def silu_both(pre):
    sigma = 0.5 * jnp.tanh(0.5 * pre) + 0.5
    act = pre * sigma
    return act, sigma * (1.0 + pre - act)


def forward(b, t, rows, loads=()):
    def layer(i, carry):
        cols = pl.ds(multiple(i, 512), 512)
        act, slope = silu_both(dot(b["x"][rows, :], b["w1"][t, :, cols]))
        b["a1"][rows, cols] = act.astype(BF16)
        b["s1"][rows, cols] = slope
        return carry

    lax.fori_loop(0, 2, layer, 0, unroll=True)
    for made in loads:
        made.wait()
    act, slope = silu_both(dot(b["a1"][rows, :], b["w2"][t]))
    b["a2"][rows, :] = act.astype(BF16)
    b["s2"][rows, :] = slope
    embedding = dot(b["a2"][rows, :], b["w3"][t])
    inv_norm = lax.rsqrt(jnp.sum(embedding * embedding, axis=1, keepdims=True) + 1.0)
    b["emb"][rows, :] = embedding
    b["inv"][rows, :] = inv_norm
    return (embedding * inv_norm).astype(BF16)


def backward(b, t, rows, unit_grad):
    embedding, inv_norm = b["emb"][rows, :], b["inv"][rows, :]
    along = jnp.sum(embedding * unit_grad, axis=1, keepdims=True)
    embed_grad = inv_norm * unit_grad - inv_norm * inv_norm * inv_norm * embedding * along
    b["eg"][rows, :] = embed_grad.astype(BF16)
    slope = dot_cols(b["eg"][rows, :], b["w3"][t]) * b["s2"][rows, :]
    b["d2"][rows, :] = slope.astype(BF16)

    def layer(i, carry):
        cols = pl.ds(multiple(i, 512), 512)
        slope = dot_cols(b["d2"][rows, :], b["w2"][t, cols, :]) * b["s1"][rows, cols]
        b["d1"][rows, cols] = slope.astype(BF16)
        return carry

    lax.fori_loop(0, 2, layer, 0, unroll=True)


def weight_gradients(b, t, rows, tower=None, add=False):
    def store(name, at, shape, value):
        if add:
            value = value + b["kept_" + name][at]
        if tower is None:
            b["kept_" + name][at] = value
        elif name == "first":
            b["g_first"][t, :, :, at[1]] = value.astype(BF16).reshape(shape)
        elif name == "second":
            b["g_second"][t, shape[0]] = value.astype(BF16).reshape(shape[1])
        else:
            b["g_third"][t] = value.astype(BF16).reshape(shape)

    def first(i, carry):
        cols = pl.ds(multiple(i, 512), 512)
        made = dot(b["xt"][:, rows], b["d1"][rows, cols])
        store("first", (slice(None), cols), (32, 16, 512), made)
        return carry

    lax.fori_loop(0, 2, first, 0, unroll=True)
    if tower is not None:
        tower.pair_first()

    def second(i, carry):
        at = pl.ds(multiple(i, 512), 512)
        made = dot(b["a1t"][at, rows], b["d2"][rows, :])
        shape = (pl.ds(multiple(i, 16), 16), (16, 2, 16, 512))
        store("second", (at, slice(None)), shape, made)
        return carry

    lax.fori_loop(0, 2, second, 0, unroll=True)
    if tower is not None:
        tower.pair_second()
    made = dot(b["a2t"][:, rows], b["eg"][rows, :])
    store("third", (slice(None), slice(None)), (4, 8, 16, 256), made)
    if tower is not None:
        tower.pair_third()


def turn_activations(b, rows):
    for name, cols in (("x", 512), ("a1", 1024), ("a2", 512)):

        def block(i, carry, name=name):
            at = pl.ds(multiple(i, 256), 256)
            turned = dot_cols(b["eye"][...], b[name][rows, at])
            b[name + "t"][at, rows] = turned.astype(BF16)
            return carry

        lax.fori_loop(0, cols // 256, block, 0, unroll=True)


def column(row):
    return jnp.broadcast_to(row, (128, 128)).T


def turn_negatives(b, u):
    for h in range(2):
        half = pl.ds(pl.multiple_of(u * 512 + h * 256, 256), 256)
        b["nt"][:, half] = dot_cols(b["eye"][...], b["n"][half, :]).astype(BF16)


def score_tile(b, pos_ids, u, i):
    at, cols = pl.ds(multiple(u, 512), 512), pl.ds(multiple(i, 512), 512)
    products = dot_cols(b["n"][at, :], b["q"][cols, :])
    logs = jnp.concatenate([b["log"][at, :]] * 4, axis=1)
    ids = jnp.concatenate([b["ids"][at, :]] * 4, axis=1)
    weights = jnp.exp2(products * (inv_temp * LOG2_E) - logs)
    rows = [pos_ids[pl.ds(i * 4 + r, 1), :].astype(F32) for r in range(4)]
    weights = jnp.where(jnp.concatenate(rows, axis=1) != ids, weights, 0.0)
    b["et"][at, cols] = weights.astype(BF16)
    b["part"][:, cols] += jnp.sum(weights.reshape(64, 8, 512), axis=0)


def step_kernel(
    query_x,
    positive_x,
    negative_x,
    q1,
    q2,
    q3,
    i1,
    i2,
    i3,
    pos_ids_in,
    pos_counts_in,
    neg_ids_in,
    neg_counts_in,
    o_query_first,
    o_query_second,
    o_query_third,
    o_item_first,
    o_item_second,
    o_item_third,
    o_scalars,
    b,
    load,
    send,
    recv,
):
    y, z, x, c = (lax.axis_index(a) for a in (AX_Y, AX_Z, AX_X, AX_C))
    me = x * 2 + c
    links = Links(send, recv, LINKS)
    phase = Phases()

    loads = [
        (negative_x, b["x"].at[pl.ds(512, 64)]),
        (i1, b["w1"].at[1]),
        (i2, b["w2"].at[1]),
        (i3, b["w3"].at[1]),
        (query_x, b["x"].at[Q_ROWS]),
        (q1, b["w1"].at[0]),
        (q2, b["w2"].at[0]),
        (q3, b["w3"].at[0]),
        (positive_x, b["x"].at[P_ROWS]),
        (pos_ids_in, b["pos_ids"]),
        (pos_counts_in, b["pos_counts"]),
        (neg_ids_in, b["neg_ids"]),
        (neg_counts_in, b["neg_counts"]),
    ]
    loads = [pltpu.make_async_copy(s, d, load.at[k]) for k, (s, d) in enumerate(loads)]
    for made in loads[:4]:
        made.start()
    barrier, peers = greet_neighbours()
    phase("load")
    for made in loads[4:]:
        made.start()

    b["x"][pl.ds(576, 64), :] = jnp.zeros((64, 512), BF16)
    b["part"][...] = jnp.zeros((8, 2048), F32)
    b["scalars"]["c_out"][...] = jnp.zeros((8, 128), F32)
    b["scalars"]["total"][...] = jnp.zeros((8, 128), F32)
    ones = lax.broadcasted_iota(jnp.int32, (256, 256), 0) == lax.broadcasted_iota(
        jnp.int32, (256, 256), 1
    )
    b["eye"][...] = jnp.where(ones, 1.0, 0.0).astype(BF16)

    loads[0].wait()
    loads[1].wait()
    phase("f_neg")
    n = b["n"]
    unit = forward(b, 1, N_ROWS, loads[2:4])

    def n_block(yy, zz):
        return n.at[pl.ds(pl.multiple_of((yy * 8 + zz) * 64, 64), 64)]

    def n_half(yy, zz, h):
        return n.at[pl.ds(pl.multiple_of((yy * 8 + zz) * 64 + h * 32, 32), 32)]

    n[pl.ds(pl.multiple_of((y * 8 + z) * 64, 64), 64), :] = unit[:64]
    phase("barrier")
    pl.semaphore_wait(barrier, peers)
    y_up, y_down = lax.rem(y + 1, 4), lax.rem(y + 3, 4)
    order = (1, 7, 2, 6, 3, 5, 4)
    n_z, n_y = {}, {}

    def n_along(*which):
        for k in which:
            n_z[k] = links.copy(n_block(y, z), n_block(y, z), {AX_Z: lax.rem(z + k, 8)})

    n_along(1, 7, 2, 6)

    def n_forward(k):
        zz = lax.rem(z - k + 8, 8)
        n_y[k] = (
            links.copy(n_block(y, zz), n_block(y, zz), {AX_Y: y_up}),
            links.copy(n_block(y, zz), n_block(y, zz), {AX_Y: y_down}),
        )

    n_forward(0)

    phase("f_query")
    for made in loads[4:8]:
        made.wait()
    q = b["q"]
    q_own = forward(b, 0, Q_ROWS)

    def q_block(xx, cc):
        return q.at[pl.ds(pl.multiple_of((xx * 2 + cc) * 256, 256), 256)]

    def q_half(xx, cc, h):
        return q.at[pl.ds(pl.multiple_of((xx * 2 + cc) * 256 + h * 128, 128), 128)]

    q[pl.ds(multiple(me, 256), 256), :] = q_own
    n_along(3, 5, 4)
    x_up, x_down, x_far = lax.rem(x + 1, 4), lax.rem(x + 3, 4), lax.rem(x + 2, 4)
    other = {AX_C: 1 - c}
    q_up, q_down = {}, {}
    for h in range(2):
        q_up[h] = links.copy(q_half(x, c, h), q_half(x, c, h), {AX_X: x_up})
        q_down[1 - h] = links.copy(q_half(x, c, 1 - h), q_half(x, c, 1 - h), {AX_X: x_down})
    q_pair = [links.copy(q_block(x, c), q_block(x, c), other)]

    phase("f_pos")
    for made in loads[8:]:
        made.wait()
    pos_ids, pos_counts, neg_ids, neg_counts = (
        b[k] for k in ("pos_ids", "pos_counts", "neg_ids", "neg_counts")
    )
    b["pos"][...] = forward(b, 1, P_ROWS)

    n_far = []

    def n_relay(*which):
        for k in which:
            zz = lax.rem(z - k + 8, 8)
            from_down, from_up = n_y[k]
            from_down.wait_recv()
            n_far.append(
                links.copy(n_half(y_down, zz, 0), n_half(y_down, zz, 0), {AX_Y: y_up})
            )
            from_up.wait_recv()
            n_far.append(
                links.copy(n_half(y_up, zz, 1), n_half(y_up, zz, 1), {AX_Y: y_down})
            )

    phase("n_fwd1")
    n_relay(0)
    for k in order[:4]:
        n_z[k].wait_recv()
        n_forward(k)
    phase("q_relay")
    q_up[0].wait_recv()
    q_low = links.copy(q_half(x_down, c, 0), q_half(x_down, c, 0), {AX_X: x_up})
    q_down[1].wait_recv()
    q_high = links.copy(q_half(x_up, c, 1), q_half(x_up, c, 1), {AX_X: x_down})
    q_up[1].wait_recv()
    q_pair.append(links.copy(q_block(x_down, c), q_block(x_down, c), other))
    q_down[0].wait_recv()
    q_pair.append(links.copy(q_block(x_up, c), q_block(x_up, c), other))

    phase("small")
    turn = b["turn"]
    turn[...] = jnp.zeros((128, 128), F32)
    turn[pl.ds(0, 16), :] = neg_ids[...].astype(F32)
    turn[pl.ds(16, 16), :] = jnp.log(neg_counts[...].astype(F32)) * LOG2_E
    turned = turn[...].T
    for j in range(16):
        b["ids"][pl.ds(j * 128, 128), :] = jnp.broadcast_to(turned[:, j : j + 1], (128, 128))
        b["log"][pl.ds(j * 128, 128), :] = jnp.broadcast_to(
            turned[:, 16 + j : 17 + j], (128, 128)
        )
    phase("n_fwd2")
    for k in order[4:]:
        n_z[k].wait_recv()
        n_forward(k)

    phase("relay_a")
    n_relay(1, 7)
    q_pair[0].wait_recv()
    phase("tile_a")
    score_tile(b, pos_ids, y, x)
    phase("relay_b")
    n_relay(2, 6)
    q_pair[1].wait_recv()
    phase("tile_b")
    score_tile(b, pos_ids, y, x_down)
    phase("relay_c")
    q_low.wait_recv()
    q_pair.append(links.copy(q_half(x_far, c, 0), q_half(x_far, c, 0), other))
    q_high.wait_recv()
    q_pair.append(links.copy(q_half(x_far, c, 1), q_half(x_far, c, 1), other))
    n_relay(3, 5)
    q_pair[2].wait_recv()
    phase("tile_c")
    score_tile(b, pos_ids, y, x_up)
    phase("relay_d")
    n_relay(4)
    phase("tiles")
    for made in q_pair[3:]:
        made.wait_recv()
    score_tile(b, pos_ids, y, x_far)

    def near_tiles(i, carry):
        score_tile(b, pos_ids, y_up, i)
        score_tile(b, pos_ids, y_down, i)
        return carry

    lax.fori_loop(0, 4, near_tiles, 0, unroll=2)
    phase("logits")
    own = b["q"][pl.ds(multiple(me, 256), 256), :].astype(F32)
    along = jnp.sum(own * b["pos"][...].astype(F32), axis=1, keepdims=True)
    logits = []
    for h in range(2):
        row = jnp.broadcast_to(along[h * 128 : (h + 1) * 128], (128, 128)).T[0:1, :]
        logits.append(row * inv_temp - jnp.log(pos_counts[h : h + 1, :].astype(F32)))

    phase("n_far")
    for made in n_far:
        made.wait_recv()
    phase("far_tiles")
    y_far = lax.rem(y + 2, 4)

    def far_tiles(i, carry):
        score_tile(b, pos_ids, y_far, i)
        return carry

    lax.fori_loop(0, 4, far_tiles, 0, unroll=True)

    phase("den")
    den_out, den_in = b["den_out"], b["den_in"]
    for j in range(16):
        den_out[pl.ds(j, 1), :] = jnp.sum(b["part"][:, j * 128 : (j + 1) * 128], axis=0, keepdims=True)
    for h in range(2):
        at = pl.ds(me * 2 + h, 1)
        den_out[at, :] = den_out[at, :] + jnp.exp(logits[h])
    sums = [links.copy(den_out, den_in.at[me], peer) for peer in group_peers()]
    den_in[me] = den_out[...]

    def turned(u, carry):
        turn_negatives(b, u)
        return carry

    lax.fori_loop(0, 4, turned, 0, unroll=True)

    phase("p_theirs")
    p_out = b["p_out"]

    def query_block(cc, i):
        cols = pl.ds(pl.multiple_of((i * 2 + cc) * 256, 256), 256)
        p_out[cc, i] = dot(b["nt"][...], b["et"][:, cols]).astype(BF16)

    def theirs(i, carry):
        query_block(1 - c, i)
        return carry

    def ours(i, carry):
        query_block(c, i)
        return carry

    lax.fori_loop(0, 4, theirs, 0, unroll=2)
    p_pair = b["p_pair"]
    pair = links.copy(p_out.at[1 - c], p_pair, other)
    phase("p_ours")
    lax.fori_loop(0, 4, ours, 0, unroll=2)
    phase("p_add")
    pair.wait_recv()
    for i in range(4):
        add_rows(p_pair.at[i], (p_pair.at[i], p_out.at[c, i]), 256, 64)
    p_x = Ring4(links, AX_X, lambda j: p_pair.at[j], 256, b["p_ring"], 128)
    p_x.start()

    phase("den_wait")
    for made in sums:
        made.wait_recv()
    total = in_order(den_in, 8)
    b["den"][...] = total
    turn[pl.ds(0, 16), :] = 1.0 / total
    turned = turn[...].T
    for j in range(16):
        at = pl.ds(j * 128, 128)
        b["qs"][at, :] = (q[at, :].astype(F32) * turned[:, j : j + 1]).astype(BF16)

    phase("g_rows")
    g_out = b["g_out"]

    def negative_rows(u):
        at = pl.ds(multiple(u, 512), 512)
        g_out[at, :] = dot(b["et"][at, :], b["qs"][...]).astype(BF16)

    g_y, g_z, g_sum = [], [], b["g_sum"]
    for h in range(2):
        cols = pl.ds(h * 128, 128)

        def cut(j, cols=cols):
            return g_out.at[pl.ds(multiple(j, 512), 512), cols]

        g_y.append(Ring4(links, AX_Y, cut, 512, b["g_ring"][h], 64))
        g_z.append(Direct(links, AX_Z, 8, b["g_z"].at[h]))
    negative_rows(g_y[0].far)
    g_y[0].start_far()
    g_y[1].start_far()
    negative_rows(g_y[0].up)
    negative_rows(g_y[0].down)
    g_y[0].start_near()

    def g_line(h):
        g_y[h].end(g_sum.at[h])
        g_z[h].start(lambda j: g_sum.at[h, pl.ds(multiple(j, 64), 64)])
    phase("p_relay")
    p_x.relay()
    phase("g_own")
    negative_rows(g_y[0].me)
    phase("g_relay0")
    g_y[0].relay()
    g_y[1].start_near()

    phase("slopes")
    losses, slopes, scales = [], [], []
    for h in range(2):
        den = b["den"][pl.ds(me * 2 + h, 1), :]
        losses.append(jnp.log(den) - logits[h])
        slope = column(jnp.exp(logits[h]) / den - 1.0) * inv_temp
        slopes.append(jnp.concatenate([slope, slope], axis=1))
        scale = column(inv_temp / den)
        scales.append(jnp.concatenate([scale, scale], axis=1))
    slopes = jnp.concatenate(slopes, axis=0)
    scales = jnp.concatenate(scales, axis=0)
    for h in range(2):
        b["scalars"]["c_out"][h + 1 : h + 2] = losses[h]
    phase("b_pos")
    own = q[pl.ds(multiple(me, 256), 256), :].astype(F32)
    backward(b, 1, P_ROWS, slopes * own)
    phase("g_relay1")
    g_y[1].relay()
    phase("turn_q")
    turn_activations(b, Q_ROWS)

    phase("p_end")
    p_x.end(b["p_sum"])
    query_grad = b["p_sum"][...].T * scales + slopes * b["pos"][...].astype(F32)
    phase("b_query")
    backward(b, 0, Q_ROWS, query_grad)
    phase("g_end0")
    g_line(0)
    phase("w_query")
    query_sum = TowerSum(links, b["sum_query"], b, 0)
    item_sum = TowerSum(links, b["sum_item"], b, 1)
    weight_gradients(b, 0, Q_ROWS, query_sum)
    phase("g_end1")
    g_line(1)

    phase("turn_n")
    turn_activations(b, N_ROWS)
    phase("q_stage1")
    query_sum.stage1()
    phase("turn_p")
    turn_activations(b, P_ROWS)
    phase("w_pos")
    weight_gradients(b, 1, P_ROWS)
    phase("q_relay1")
    query_sum.relay1()

    phase("g_z")
    halves = []
    for h in range(2):
        g_z[h].wait()
        total = g_sum[h, pl.ds(multiple(z, 64), 64), :].astype(F32)
        for k in range(1, 8):
            total = total + b["g_z"][h, lax.rem(z + k, 8)].astype(F32)
        halves.append(total)
    total = jnp.concatenate(halves, axis=1)
    total = jnp.concatenate([total * inv_temp, jnp.zeros((64, 256), F32)], axis=0)
    phase("b_neg")
    backward(b, 1, N_ROWS, total)
    phase("w_item")
    weight_gradients(b, 1, N_ROWS, item_sum, add=True)
    phase("i_stage1")
    item_sum.stage1()
    phase("q_stage2")
    query_sum.stage2()
    query_sum.third1()
    item_sum.third1()
    phase("i_relay1")
    item_sum.relay1()
    phase("q_stage3")
    query_sum.stage3()
    query_sum.third2()
    phase("i_stage2")
    item_sum.stage2()
    phase("q_third3")
    query_sum.third3()
    item_sum.third2()
    phase("i_stage3")
    item_sum.stage3()
    phase("q_last")
    item_sum.third3()
    squares = query_sum.last()
    query_sum.spread()
    phase("i_last")
    squares = squares + item_sum.last()
    scalars = Scalars(links, b["scalars"])
    scalars.start(squares)
    phase("group")
    scalars.over_plane()
    item_sum.spread()
    phase("pieces")
    stage = b["stage"]
    query_sum.collect(*stage[:3])
    item_sum.collect(*stage[3:])
    stores = [
        pltpu.make_async_copy(stage[k], result, load.at[13 + k])
        for k, result in enumerate(
            (
                o_query_first,
                o_query_second,
                o_query_third,
                o_item_first,
                o_item_second,
                o_item_third,
            )
        )
    ]
    for made in stores:
        made.start()
    phase("finish")
    links.finish()
    phase("plane")
    total = scalars.end()
    row = lax.broadcasted_iota(jnp.int32, (8, 128), 0)
    norm = jnp.sqrt(jnp.sum(jnp.where(row == 0, total, 0.0), keepdims=True))
    factor = clip_norm / jnp.maximum(norm, clip_norm)
    o_scalars[0] = jnp.broadcast_to(factor, (8, 128))
    o_scalars[1] = jnp.broadcast_to(jnp.sum(jnp.where((row == 1) | (row == 2), total, 0.0), keepdims=True), (8, 128))
    for made in stores:
        made.wait()
    phase(None)


def clip_kernel(*refs):
    scalars, raw, clipped, loss = refs[0], refs[1:7], refs[7:13], refs[13]
    factor = scalars[0, 0:1, 0:1]
    for source, result in zip(raw, clipped):
        result[...] = source[...] * factor
    loss[...] = scalars[1, 0:1, 0:1] * (1.0 / QUERIES)


def per_device(
    query_features,
    positive_features,
    negative_features,
    positive_ids,
    positive_counts,
    negative_ids,
    negative_counts,
    query_first,
    query_second,
    query_third,
    item_first,
    item_second,
    item_third,
):
    vmem = pl.BlockSpec(memory_space=pltpu.VMEM)
    anywhere = pl.BlockSpec(memory_space=pl.ANY)
    tower = (
        jax.ShapeDtypeStruct((16, 1024), F32),
        jax.ShapeDtypeStruct((32, 512), F32),
        jax.ShapeDtypeStruct((16, 256), F32),
    )
    *raw, scalars = pl.pallas_call(
        step_kernel,
        out_shape=tower + tower + (jax.ShapeDtypeStruct((2, 8, 128), F32),),
        in_specs=[anywhere] * 13,
        out_specs=(anywhere,) * 6 + (vmem,),
        scratch_shapes=[
            STEP_BUFS,
            pltpu.SemaphoreType.DMA((19,)),
            pltpu.SemaphoreType.DMA((LINKS,)),
            pltpu.SemaphoreType.DMA((LINKS,)),
        ],
        compiler_params=pltpu.CompilerParams(
            collective_id=0, has_side_effects=True, vmem_limit_bytes=60 * 1024 * 1024
        ),
        name="training_step",
    )(
        query_features,
        positive_features,
        negative_features,
        query_first,
        query_second,
        query_third,
        item_first,
        item_second,
        item_third,
        positive_ids.reshape(16, 128),
        positive_counts.reshape(2, 128),
        negative_ids.reshape(16, 128),
        negative_counts.reshape(16, 128),
    )
    *clipped, loss = pl.pallas_call(
        clip_kernel,
        out_shape=tower + tower + (jax.ShapeDtypeStruct((1, 1), F32),),
        in_specs=[vmem] * 7,
        out_specs=(vmem,) * 7,
        name="clip",
    )(scalars, *raw)
    return (loss.reshape(()), *clipped)


def solution(mesh):
    torus = Mesh(mesh.devices.reshape(4, 8, 4, 2), DP_NEG)
    placed = (
        P(DP_NEG, None),
        P(DP_NEG, None),
        P(NEG_DP, None),
        P(DP),
        P(DP_NEG),
        P(NEG),
        P(NEG),
        P(),
        P(),
        P(),
        P(),
        P(),
        P(),
    )
    return jax.shard_map(
        per_device,
        mesh=torus,
        in_specs=placed,
        out_specs=(P(),) + (P(DP, None),) * 6,
        check_vma=False,
    )
```
